128 devices in a mesh: dp: 32 (over x, y, core), group: 4 (over z).
Axes of the slice: x: 4, y: 4, z: 4, core: 2. Of those that a mesh axis runs over, the one named last changes fastest.
Arguments:
- images: bfloat16 [16384, 512], P(('dp', 'group')), may hold values from -1 to 1
- texts: bfloat16 [16384, 512], P(('dp', 'group')), may hold values from -1 to 1
- log_scale: float32 [], replicated, may hold values from 2 to 2.7
Outputs:
- grad_images: bfloat16 [16384, 512], P(('dp', 'group'))
- grad_texts: bfloat16 [16384, 512], P(('dp', 'group'))
- loss: float32 [], replicated
- grad_scale: float32 [], replicated
The draws below stay inside these ranges and needn't reach their ends.
All inputs are finite; a program needn't handle non-finite values.
Results may differ from the reference program's by a relative error of at most 0.0013.
The reference program's roundings to bfloat16 on the way (of `weights_low`) count: a program that leaves them out, or rounds other values in their place, can miss the bound.
Values may be sent and summed in bfloat16 or wider, within the bound.
A program may use at most 128 MiB of HBM per device.

```python
import jax
import jax.numpy as jnp
from jax import lax

D = 512
B_DEV = 128
N = 16384


def draw_pair(key):
    spread_dims = jnp.exp(jax.random.uniform(jax.random.fold_in(key, 17), (1, D), jnp.float32, -0.693, 0.693))
    spread_dims = spread_dims / jnp.sqrt(jnp.mean(spread_dims * spread_dims))
    base = jnp.clip(0.05 * spread_dims * jax.random.normal(jax.random.fold_in(key, 11), (N, D), jnp.float32), -0.5, 0.5)
    noise = jnp.clip(0.05 * spread_dims * jax.random.normal(jax.random.fold_in(key, 12), (N, D), jnp.float32), -0.5, 0.5)
    paired = 0.3 * base + 0.95 * noise
    common = 0.05 * jax.random.rademacher(jax.random.fold_in(key, 16), (1, D), jnp.float32)
    image_share = jax.random.uniform(jax.random.fold_in(key, 18), (N, 1), jnp.float32, 0.1, 0.4)
    text_share = jax.random.uniform(jax.random.fold_in(key, 19), (N, 1), jnp.float32, 0.1, 0.4)
    base = base + image_share * common
    paired = paired + text_share * common
    return (jnp.clip(base, -1.0, 1.0), jnp.clip(paired, -1.0, 1.0))


def draw_images(key, part):
    return draw_pair(key)[0].astype(jnp.bfloat16)


def draw_texts(key, part):
    return draw_pair(key)[1].astype(jnp.bfloat16)


def setup_inputs(seed: int = 0) -> dict:
    streams_of = jax.random.split(jax.random.key(seed), 4)
    images = draw_images(jax.random.fold_in(streams_of[3], 71), 0)
    texts = draw_texts(jax.random.fold_in(streams_of[3], 71), 0)
    log_scale = jnp.clip(jax.random.uniform(streams_of[2], (), jnp.float32, 2.0, 2.7), 2.0, 2.7)
    return dict(images=images, texts=texts, log_scale=log_scale)


def reference(images, texts, log_scale):
    pair_total = images.shape[0]
    block_rows = B_DEV
    block_count = pair_total // block_rows
    logit_scale = jnp.exp(log_scale)
    columns = jnp.arange(pair_total).astype(jnp.int32)

    def logits_at(block_index):
        first_row = (block_index * block_rows).astype(jnp.int32)
        image_rows = lax.dynamic_slice_in_dim(images, first_row, block_rows, 0)
        logits = logit_scale * jnp.dot(image_rows, texts.T, preferred_element_type=jnp.float32)
        return image_rows, first_row, logits

    def first_pass(carry, block_index):
        col_top, col_sum = carry
        image_rows, first_row, logits = logits_at(block_index)
        row_top = jnp.max(logits, axis=1)
        row_lse = row_top + jnp.log(jnp.sum(jnp.exp(logits - row_top[:, None]), axis=1))
        paired = jnp.diagonal(lax.dynamic_slice_in_dim(logits, first_row, block_rows, 1))
        new_top = jnp.maximum(col_top, jnp.max(logits, axis=0))
        col_sum = col_sum * jnp.exp(col_top - new_top) + jnp.sum(jnp.exp(logits - new_top[None, :]), axis=0)
        return (new_top, col_sum), (row_lse, paired)

    start_carry = (jnp.full((pair_total,), -1e30, jnp.float32), jnp.zeros((pair_total,), jnp.float32))
    indices = jnp.arange(block_count).astype(jnp.int32)
    (col_top, col_sum), (row_lse, paired) = lax.scan(first_pass, start_carry, indices)
    col_lse = col_top + jnp.log(col_sum)

    def second_pass(carry, inputs):
        text_sum, scale_sum = carry
        block_index, block_lse = inputs
        image_rows, first_row, logits = logits_at(block_index)
        own_pairs = (columns[None, :] == (first_row + jnp.arange(block_rows).astype(jnp.int32))[:, None]).astype(jnp.float32)
        grad_block = 0.5 * (jnp.exp(logits - block_lse[:, None]) + jnp.exp(logits - col_lse[None, :])) - own_pairs
        scale_sum = scale_sum + jnp.sum(grad_block * logits)
        weights_low = grad_block.astype(jnp.bfloat16)
        image_grad = logit_scale * jnp.dot(weights_low, texts, preferred_element_type=jnp.float32)
        text_sum = text_sum + jnp.dot(weights_low.T, image_rows, preferred_element_type=jnp.float32)
        return (text_sum, scale_sum), image_grad.astype(jnp.bfloat16)

    start_two = (jnp.zeros(texts.shape, jnp.float32), jnp.zeros((), jnp.float32))
    (text_sum, scale_sum), image_blocks = lax.scan(second_pass, start_two, (indices, row_lse))
    grad_images = image_blocks.reshape(pair_total, images.shape[1])
    grad_texts = (logit_scale * text_sum).astype(jnp.bfloat16)
    loss = (jnp.sum(row_lse) + jnp.sum(col_lse) - 2.0 * jnp.sum(paired)) / (2.0 * pair_total)
    grad_scale = scale_sum / pair_total
    return grad_images, grad_texts, loss, grad_scale
```

```python
import functools
import math

import jax
import jax.numpy as jnp
from jax import lax
from jax.experimental import pallas as pl
from jax.experimental.pallas import tpu as pltpu
from jax.sharding import Mesh
from jax.sharding import PartitionSpec as P

AXES = ("x", "y", "core", "z")
CUBE = ("x", "y", "z")
MESH = pl.DeviceIdType.MESH
ROWS = 128
LOG2E = math.log2(math.e)
LN2 = math.log(2.0)
NT = (((1,), (1,)), ((), ()))


def kernel(
    dims, total,
    log_scale, images, texts,
    gi_out, gt_out, stats_out,
    X, XT, T, L, W, RM, RS, CM, CS, RL, CL, RREP, CROW,
    PI, RI, PT, RTC, RT, ST,
    local_sem, xs, xr, ts, tr, ds, dr, rls, rlr, cls, clr, pis, pir, pcs, pcr, pts, ptr, sts, str_,
):
    nd = len(dims)
    nb = 2**nd
    rows = nb * ROWS
    me = {a: lax.axis_index(a) for a in AXES}
    core = me["core"]

    def peer(mask, kind, flip):
        ident = {}
        for d, a in enumerate(dims):
            if mask >> d & 1:
                c = me[a]
                ident[a] = c + 1 - 2 * (c % 2) if kind == "A" else 3 - c
        if flip:
            ident["core"] = 1 - core
        return ident

    def spot(mask, kind):
        at = 0
        for d, a in enumerate(dims):
            bit = me[a] % 2 if kind == "A" else me[a] // 2
            at = at + 2**d * (1 - bit if mask >> d & 1 else bit)
        return at

    def send(src, dst, s, r, where):
        return pltpu.make_async_remote_copy(
            src_ref=src, dst_ref=dst, send_sem=s, recv_sem=r, device_id=where, device_id_type=MESH
        )

    def block(ref, m, n=ROWS):
        return ref.at[pl.ds(m * n, n)]

    ci = pltpu.make_async_copy(images, block(X, 0), local_sem.at[0])
    ct = pltpu.make_async_copy(texts, block(T, 0), local_sem.at[1])
    ci.start()
    ct.start()
    barrier = pltpu.get_barrier_semaphore()
    others = [(m, "A", False) for m in range(1, nb)]
    others += [(m, "B", f) for m in range(nb) for f in (False, True) if m or f]
    for o in others:
        pl.semaphore_signal(barrier, inc=1, device_id=peer(*o), device_id_type=MESH)
    ci.wait()
    ct.wait()
    pl.semaphore_wait(barrier, len(others))

    xc = [send(block(X, 0), block(X, m), xs.at[m], xr.at[m], peer(m, "A", False)) for m in range(1, nb)]
    tc = [send(block(T, 0), block(T, 2 * m), ts.at[m], tr.at[m], peer(m, "B", False)) for m in range(1, nb)]
    dc = [send(block(T, 2 * m), block(T, 2 * m + 1), ds.at[m], dr.at[m], peer(0, "B", True)) for m in range(nb)]
    dc[0].start()
    for a, b in zip(xc, tc):
        a.start()
        b.start()
    for m in range(1, nb):
        tc[m - 1].wait_recv()
        dc[m].start()
    for c in xc:
        c.wait_recv()
    for c in dc:
        c.wait_recv()
    for c in xc + tc + dc:
        c.wait_send()

    scale = jnp.exp(jnp.full((1, 128), log_scale[0], jnp.float32))
    scale_two = jnp.concatenate([scale * LOG2E] * 2, axis=1)
    XT[...] = X[...].T

    RM[...] = jnp.full(RM.shape, -3e38, jnp.float32)

    def logits(m, _):
        cols = pl.ds(pl.multiple_of(m * 256, 256), 256)
        v = lax.dot_general(X[...], T[cols, :], NT, preferred_element_type=jnp.float32) * scale_two
        L[:, cols] = v
        RM[...] = jnp.maximum(RM[...], jnp.maximum(v[:, :128], v[:, 128:]))
        CM[:, cols] = jnp.max(v, axis=0, keepdims=True)
        return 0

    lax.fori_loop(0, nb, logits, 0)

    def spread(m, _):
        at = pl.ds(pl.multiple_of(m * 128, 128), 128)
        RM[at, :] = jnp.broadcast_to(jnp.max(RM[at, :], axis=1, keepdims=True), (128, 128))
        return 0

    lax.fori_loop(0, nb, spread, 0)
    RS[...] = jnp.zeros(RS.shape, jnp.float32)

    def sums(m, _):
        cols = pl.ds(pl.multiple_of(m * 256, 256), 256)
        cm = CM[:, cols]

        def strip(i, cs):
            at = pl.ds(pl.multiple_of(i * 64, 64), 64)
            v = L[at, cols]
            rm = RM[at, :]
            er0 = jnp.exp2(v[:, :128] - rm)
            er1 = jnp.exp2(v[:, 128:] - rm)
            RS[at, :] = RS[at, :] + (er0 + er1)
            ec = jnp.exp2(v - cm)
            return cs + jnp.sum(ec.reshape(8, 8, 256), axis=0)

        cs = lax.fori_loop(0, rows // 64, strip, jnp.zeros((8, 256), jnp.float32))
        CS[:, cols] = jnp.sum(cs, axis=0, keepdims=True)
        return 0

    lax.fori_loop(0, nb, sums, 0)

    for m in range(nb):
        at = slice(m * 128, (m + 1) * 128)
        top = jnp.max(RM[at, :].T, axis=0, keepdims=True)
        part = jnp.sum(RS[at, :].T, axis=0, keepdims=True)
        RL[0, pl.ds(spot(m, "A"), 1), :] = top + jnp.log2(part)
    ccol = CM[...] + jnp.log2(CS[...])
    for m in range(nb):
        for f in range(2):
            at = (2 * m + f) * 128
            line = (1 - core if f else core) * nb + spot(m, "B")
            CL[0, pl.ds(line, 1), :] = ccol[:, at : at + 128]
    rc = [send(RL.at[0], RL.at[m], rls.at[m], rlr.at[m], peer(m, "A", False)) for m in range(1, nb)]
    cc = [
        send(CL.at[0], CL.at[2 * m + f], cls.at[2 * m + f], clr.at[2 * m + f], peer(m, "B", f == 1))
        for m in range(nb) for f in range(2) if m or f
    ]
    for c in cc + rc:
        c.start()
    for c in cc + rc:
        c.wait_recv()
    for c in cc + rc:
        c.wait_send()

    def joined(parts):
        top = functools.reduce(jnp.maximum, parts)
        return top + jnp.log2(functools.reduce(jnp.add, [jnp.exp2(p - top) for p in parts]))

    row_all = joined([RL[m] for m in range(nb)])
    col_all = joined([CL[m] for m in range(2 * nb)])
    RL[0] = row_all
    CL[0] = col_all
    for m in range(nb):
        line = RL[0, pl.ds(spot(m, "A"), 1), :]
        RREP[m * 128 : (m + 1) * 128, :] = jnp.broadcast_to(line + 1.0, (128, 128)).T
        for f in range(2):
            at = (2 * m + f) * 128
            CROW[:, at : at + 128] = CL[0, pl.ds((1 - core if f else core) * nb + spot(m, "B"), 1), :] + 1.0

    eye = (lax.broadcasted_iota(jnp.int32, (128, 128), 0) == lax.broadcasted_iota(jnp.int32, (128, 128), 1))
    own = L[:128, :128]
    paired = jnp.sum(jnp.where(eye, own, 0.0))
    loss_part = LN2 * (
        jnp.sum(RL[0, pl.ds(spot(0, "A"), 1), :]) + jnp.sum(CL[0, pl.ds(core * nb + spot(0, "B"), 1), :]) - 2.0 * paired
    )

    def weigh(m, acc):
        cols = pl.ds(pl.multiple_of(m * 256, 256), 256)
        cl = CROW[:, cols]

        def strip(i, acc):
            at = pl.ds(pl.multiple_of(i * 64, 64), 64)
            v = L[at, cols]
            rl = RREP[at, :]
            rl = jnp.concatenate([rl, rl], axis=1)
            w = jnp.exp2(v - rl) + jnp.exp2(v - cl)
            W[at, cols] = w.astype(jnp.bfloat16)
            return acc + jnp.sum((w * v).reshape(8, 8, 256), axis=0)

        return lax.fori_loop(0, rows // 64, strip, acc)

    acc = lax.fori_loop(0, nb, weigh, jnp.zeros((8, 256), jnp.float32))
    w = jnp.exp2(own - RREP[:128, :]) + jnp.exp2(own - CROW[:, :128])
    W[:128, :128] = (w - eye.astype(jnp.float32)).astype(jnp.bfloat16)
    scale_part = LN2 * (jnp.sum(acc) - paired)

    def image_grad(i, _):
        at = pl.ds(pl.multiple_of(i * 256, 256), 256)
        PI[at, :] = jnp.dot(W[at, :], T[...], preferred_element_type=jnp.float32)
        return 0

    lax.fori_loop(0, rows // 256, image_grad, 0)
    ic = [send(block(PI, m), block(RI, m), pis.at[m], pir.at[m], peer(m, "A", False)) for m in range(1, nb)]
    for c in ic:
        c.start()

    def text_grad(m, _):
        cols = pl.ds(pl.multiple_of(m * 256, 256), 256)
        v = jnp.dot(XT[...], W[:, cols], preferred_element_type=jnp.float32)
        PT[0, m] = v[:, :128]
        PT[1, m] = v[:, 128:]
        return 0

    lax.fori_loop(0, nb, text_grad, 0)
    pc = [send(PT.at[1, m], RTC.at[m], pcs.at[m], pcr.at[m], peer(0, "B", True)) for m in range(nb)]
    oc = [send(PT.at[0, m], RT.at[m], pts.at[m], ptr.at[m], peer(m, "B", False)) for m in range(1, nb)]
    for m in reversed(range(nb)):
        pc[m].start()
    for m in reversed(range(nb)):
        pc[m].wait_recv()
        PT[0, m] = PT[0, m] + RTC[m]
        if m:
            oc[m - 1].start()

    line = lax.broadcasted_iota(jnp.int32, (8, 128), 0)
    tile = jnp.where(line == 0, loss_part, jnp.where(line == 1, scale_part, 0.0))
    base = 0
    for kind, masks, flip in (("A", range(1, nb), False), ("B", range(1, nb), False), ("B", (0,), True)):
        ST[base] = tile
        copies = [
            send(ST.at[base], ST.at[base + 1 + i], sts.at[base + i], str_.at[base + i], peer(m, kind, flip))
            for i, m in enumerate(masks)
        ]
        for c in copies:
            c.start()
        for c in copies:
            c.wait_recv()
        for i in range(len(copies)):
            tile = tile + ST[base + 1 + i]
        for c in copies:
            c.wait_send()
        base += 1 + len(copies)
    stats_out[...] = jnp.where(line == 0, tile * (0.5 / total), tile * (1.0 / total))

    for c in ic:
        c.wait_recv()
    gi = PI[:128, :]
    for m in range(1, nb):
        gi = gi + RI[m * 128 : (m + 1) * 128, :]
    gi_out[...] = (gi * scale[:, :1]).astype(jnp.bfloat16)
    for c in oc:
        c.wait_recv()
    gt = PT[0, 0]
    for m in range(1, nb):
        gt = gt + RT[m]
    gt_out[...] = (gt * scale).T.astype(jnp.bfloat16)
    for c in ic + pc + oc:
        c.wait_send()


def body(dims, total, images, texts, log_scale):
    nb = 2 ** len(dims)
    f32, bf16 = jnp.float32, jnp.bfloat16
    vm, dma = pltpu.VMEM, pltpu.SemaphoreType.DMA
    width = images.shape[1]
    rows, cols = nb * ROWS, 2 * nb * ROWS
    gi, gt, stats = pl.pallas_call(
        functools.partial(kernel, dims, total),
        out_shape=(
            jax.ShapeDtypeStruct(images.shape, bf16),
            jax.ShapeDtypeStruct(texts.shape, bf16),
            jax.ShapeDtypeStruct((8, 128), f32),
        ),
        in_specs=[
            pl.BlockSpec(memory_space=pltpu.SMEM),
            pl.BlockSpec(memory_space=pl.ANY),
            pl.BlockSpec(memory_space=pl.ANY),
        ],
        out_specs=(pl.BlockSpec(memory_space=vm),) * 3,
        scratch_shapes=[
            vm((rows, width), bf16), vm((width, rows), bf16), vm((cols, width), bf16),
            vm((rows, cols), f32), vm((rows, cols), bf16),
            vm((rows, 128), f32), vm((rows, 128), f32), vm((1, cols), f32), vm((1, cols), f32),
            vm((nb, nb, 128), f32), vm((2 * nb, 2 * nb, 128), f32), vm((rows, 128), f32), vm((1, cols), f32),
            vm((rows, width), f32), vm((rows, width), f32),
            vm((2, nb, width, 128), f32), vm((nb, width, 128), f32), vm((nb, width, 128), f32),
            vm((2 * nb + 2, 8, 128), f32),
            dma((2,)), dma((nb,)), dma((nb,)), dma((nb,)), dma((nb,)), dma((nb,)), dma((nb,)),
            dma((nb,)), dma((nb,)), dma((2 * nb,)), dma((2 * nb,)),
            dma((nb,)), dma((nb,)), dma((nb,)), dma((nb,)), dma((nb,)), dma((nb,)),
            dma((2 * nb + 2,)), dma((2 * nb + 2,)),
        ],
        compiler_params=pltpu.CompilerParams(
            collective_id=0, has_side_effects=True, vmem_limit_bytes=60 * 2**20
        ),
        name="contrastive",
    )(log_scale.reshape(1), images, texts)
    return gi, gt, stats[0, 0], stats[1, 0]


def solution(mesh):
    return build(Mesh(mesh.devices.reshape(4, 4, 2, 4), AXES))


def build(split):
    dims = tuple(a for a in CUBE if split.shape[a] == 4)
    placed = P(AXES, None)
    return jax.shard_map(
        functools.partial(body, dims, ROWS * split.size),
        mesh=split,
        in_specs=(placed, placed, P()),
        out_specs=(placed, placed, P(), P()),
        check_vma=False,
    )
```

```python
import functools
import math

import jax
import jax.numpy as jnp
from jax import lax
from jax.experimental import pallas as pl
from jax.experimental.pallas import tpu as pltpu
from jax.sharding import Mesh
from jax.sharding import PartitionSpec as P

AXES = ("x", "y", "core", "z")
CUBE = ("x", "y", "z")
MESH = pl.DeviceIdType.MESH
ROWS = 128
LOG2E = math.log2(math.e)
LN2 = math.log(2.0)
NT = (((1,), (1,)), ((), ()))


class Cube:
    def __init__(self, n):
        self.n = n
        self.order = sorted(range(2**n), key=lambda m: (bin(m).count("1"), m))
        self.pos = {m: i for i, m in enumerate(self.order)}
        self.level = {m: bin(m).count("1") for m in self.order}
        self.pieces = range(n)

    def hop(self, p, m):
        return next(k % self.n for k in range(p, p + self.n) if m >> (k % self.n) & 1)

    def children(self, p, m):
        more = [(k, m | 1 << k) for k in range(self.n) if not m >> k & 1]
        return [c for k, c in more if self.hop(p, c) == k]

    def turns(self):
        seen = []
        for q in (1, -1, 0):
            if q % self.n not in seen:
                seen.append(q % self.n)
        return seen


def cut(total, n, unit):
    units = total // unit
    ends = [-(-units * i // n) * unit for i in range(n + 1)]
    return [(a, b - a) for a, b in zip(ends, ends[1:])]


def kernel(
    dims, total,
    log_scale, images, texts,
    gi_out, gt_out, stats_out,
    X, XT, T, L, W, RM, RS, CM, CS, RL, CL, RREP, CROW,
    PI, RI, PT, RTC, RT, ST,
    local_sem, xs, xr, ts, tr, ds, dr, rls, rlr, cls, clr, pis, pir, pcs, pcr, pts, ptr, sts, str_,
):
    nd = len(dims)
    nb = 2**nd
    rows = nb * ROWS
    cube = Cube(nd)
    order, pos = cube.order, cube.pos
    me = {a: lax.axis_index(a) for a in AXES}
    core = me["core"]

    def peer(mask, kind, flip=False):
        ident = {}
        for d, a in enumerate(dims):
            if mask >> d & 1:
                c = me[a]
                ident[a] = c + 1 - 2 * (c % 2) if kind == "A" else 3 - c
        if flip:
            ident["core"] = 1 - core
        return ident

    def spot(mask, kind):
        at = 0
        for d, a in enumerate(dims):
            bit = me[a] % 2 if kind == "A" else me[a] // 2
            at = at + 2**d * (1 - bit if mask >> d & 1 else bit)
        return at

    def send(src, dst, s, r, where):
        return pltpu.make_async_remote_copy(
            src_ref=src, dst_ref=dst, send_sem=s, recv_sem=r, device_id=where, device_id_type=MESH
        )

    with jax.named_scope("enter"):
        ci = pltpu.make_async_copy(images, X.at[pl.ds(0, ROWS)], local_sem.at[0])
        ct = pltpu.make_async_copy(texts, T.at[pl.ds(0, ROWS)], local_sem.at[1])
        ci.start()
        ct.start()
        barrier = pltpu.get_barrier_semaphore()
        others = [(m, "A", False) for m in range(1, nb)]
        others += [(m, "B", f) for m in range(nb) for f in (False, True) if m or f]
        for o in others:
            pl.semaphore_signal(barrier, inc=1, device_id=peer(*o), device_id_type=MESH)
        RM[...] = jnp.full(RM.shape, -3e38, jnp.float32)
        RS[...] = jnp.zeros(RS.shape, jnp.float32)
        CM[...] = jnp.full(CM.shape, -3e38, jnp.float32)
        scale = jnp.exp(jnp.full((1, 128), log_scale[0], jnp.float32))
        scale_two = jnp.concatenate([scale * LOG2E] * 2, axis=1)
        ci.wait()
        ct.wait()
        pl.semaphore_wait(barrier, len(others))

    gp = cut(ROWS, nd, 16)
    started = []

    def go(c):
        c.start()
        started.append(c)

    def xmsg(m, p):
        k = cube.hop(p, m)
        a, n = gp[p]
        src = X.at[pl.ds(pos[m ^ 1 << k] * ROWS + a, n)]
        return send(src, X.at[pl.ds(pos[m] * ROWS + a, n)], xs.at[m, p], xr.at[m, p], peer(1 << k, "A"))

    def tmsg(m, p):
        k = cube.hop(p, m)
        a, n = gp[p]
        src = T.at[pl.ds(pos[m ^ 1 << k] * 2 * ROWS + a, n)]
        return send(src, T.at[pl.ds(pos[m] * 2 * ROWS + a, n)], ts.at[m, p], tr.at[m, p], peer(1 << k, "B"))

    def dmsg(m, p):
        a, n = gp[p]
        at = pos[m] * 2 * ROWS + a
        return send(T.at[pl.ds(at, n)], T.at[pl.ds(at + ROWS, n)], ds.at[m, p], dr.at[m, p], peer(0, "B", True))

    def pass_on(events):
        for m, p in events:
            xmsg(m, p).wait_recv()
        nxt = [(c, p) for m, p in events for c in cube.children(p, m)]
        nxt.sort(key=lambda e: not cube.children(e[1], e[0]))
        for e in nxt:
            go(xmsg(*e))
        for m, p in events:
            tmsg(m, p).wait_recv()
        for e in nxt:
            go(tmsg(*e))
        for e in events:
            go(dmsg(*e))

    def logits(r0, r1, c0, c1):
        def step(i, _):
            cols = pl.ds(pl.multiple_of(i * 256, 256), 256)
            v = lax.dot_general(X[r0:r1, :], T[cols, :], NT, preferred_element_type=jnp.float32) * scale_two
            L[r0:r1, cols] = v
            RM[r0:r1, :] = jnp.maximum(RM[r0:r1, :], jnp.maximum(v[:, :128], v[:, 128:]))
            CM[:, cols] = jnp.maximum(CM[:, cols], jnp.max(v, axis=0, keepdims=True))
            return 0

        lax.fori_loop(c0, c1, step, 0)

    def partner_texts(masks):
        for m in masks:
            for p in cube.pieces:
                dmsg(m, p).wait_recv()

    with jax.named_scope("gather"):
        for p in cube.pieces:
            go(dmsg(0, p))
        for q in cube.turns():
            for k in range(nd):
                go(xmsg(1 << k, (k + q) % nd))
                go(tmsg(1 << k, (k + q) % nd))
        groups = [[(1 << k, (k + q) % nd) for k in range(nd)] for q in cube.turns()]
        for g in groups:
            pass_on(g)
        levels = [[m for m in order if cube.level[m] == i] for i in range(nd + 1)]
    done = 0
    for lev in range(1, nd + 1):
        with jax.named_scope(f"gather{lev}"):
            have = sum(len(levels[i]) for i in range(lev))
            fresh = done
            if lev > 1:
                events = [(m, p) for m in levels[lev] for p in cube.pieces]
                deep = [e for e in events if cube.children(e[1], e[0])]
                if deep:
                    pass_on(deep)
                pass_on([e for e in events if e not in deep])
                have += len(levels[lev])
                partner_texts(levels[lev])
            else:
                have += len(levels[1])
                partner_texts(levels[0] + levels[1])
        with jax.named_scope(f"logits{lev}"):
            if done:
                logits(done * ROWS, have * ROWS, 0, done)
            logits(0, have * ROWS, done, have)
            done = have

    with jax.named_scope("sums"):
        def spread(m, _):
            at = pl.ds(pl.multiple_of(m * 128, 128), 128)
            RM[at, :] = jnp.broadcast_to(jnp.max(RM[at, :], axis=1, keepdims=True), (128, 128))
            return 0

        lax.fori_loop(0, nb, spread, 0)
        strip_rows = 256

        def sums(m, _):
            cols = pl.ds(pl.multiple_of(m * 256, 256), 256)
            cm = CM[:, cols]

            def strip(i, cs):
                at = pl.ds(pl.multiple_of(i * strip_rows, strip_rows), strip_rows)
                v = L[at, cols]
                rm = RM[at, :]
                er0 = jnp.exp2(v[:, :128] - rm)
                er1 = jnp.exp2(v[:, 128:] - rm)
                RS[at, :] = RS[at, :] + (er0 + er1)
                ec = jnp.exp2(v - cm)
                return cs + jnp.sum(ec.reshape(strip_rows // 8, 8, 256), axis=0)

            cs = lax.fori_loop(0, rows // strip_rows, strip, jnp.zeros((8, 256), jnp.float32))
            CS[:, cols] = jnp.sum(cs, axis=0, keepdims=True)
            return 0

        lax.fori_loop(0, nb, sums, 0)

    with jax.named_scope("lse"):
        ccol = CM[...] + jnp.log2(CS[...])
        for m in order:
            for f in range(2):
                at = (2 * pos[m] + f) * 128
                line = (1 - core if f else core) * nb + spot(m, "B")
                CL[0, pl.ds(line, 1), :] = ccol[:, at : at + 128]
        cc = [
            send(CL.at[0], CL.at[2 * m + f], cls.at[2 * m + f], clr.at[2 * m + f], peer(m, "B", f == 1))
            for m in reversed(order) for f in range(2) if m or f
        ]
        for c in cc:
            c.start()
        for m in order:
            at = slice(pos[m] * 128, (pos[m] + 1) * 128)
            top = jnp.max(RM[at, :].T, axis=0, keepdims=True)
            part = jnp.sum(RS[at, :].T, axis=0, keepdims=True)
            RL[0, pl.ds(spot(m, "A"), 1), :] = top + jnp.log2(part)
        rc = [send(RL.at[0], RL.at[m], rls.at[m], rlr.at[m], peer(m, "A")) for m in reversed(order[1:])]
        for c in rc:
            c.start()
    with jax.named_scope("turn"):
        XT[...] = X[...].T
        for c in started:
            c.wait_send()
    with jax.named_scope("lsewait"):
        for c in cc + rc:
            c.wait_recv()
        for c in cc + rc:
            c.wait_send()

    with jax.named_scope("join"):
        def joined(parts):
            top = functools.reduce(jnp.maximum, parts)
            return top + jnp.log2(functools.reduce(jnp.add, [jnp.exp2(p - top) for p in parts]))

        RL[0] = joined([RL[m] for m in range(nb)])
        CL[0] = joined([CL[m] for m in range(2 * nb)])
        for m in order:
            line = RL[0, pl.ds(spot(m, "A"), 1), :]
            RREP[pos[m] * 128 : (pos[m] + 1) * 128, :] = jnp.broadcast_to(line + 1.0, (128, 128)).T
            for f in range(2):
                at = (2 * pos[m] + f) * 128
                CROW[:, at : at + 128] = CL[0, pl.ds((1 - core if f else core) * nb + spot(m, "B"), 1), :] + 1.0
        eye = lax.broadcasted_iota(jnp.int32, (128, 128), 0) == lax.broadcasted_iota(jnp.int32, (128, 128), 1)
        own = L[:128, :128]
        paired = jnp.sum(jnp.where(eye, own, 0.0))
        loss_part = LN2 * (
            jnp.sum(RL[0, pl.ds(spot(0, "A"), 1), :])
            + jnp.sum(CL[0, pl.ds(core * nb + spot(0, "B"), 1), :])
            - 2.0 * paired
        )

    ip = cut(ROWS, nd, 8)
    tp = cut(XT.shape[0], nd, 8)

    def imsg(m, p):
        k = cube.hop(p, m)
        a, n = ip[p]
        at = pl.ds(pos[m] * ROWS + a, n)
        return send(PI.at[at], RI.at[at], pis.at[m, p], pir.at[m, p], peer(1 << k, "A"))

    def omsg(m, p):
        k = cube.hop(p, m)
        a, n = tp[p]
        at = pl.ds(a, n)
        return send(PT.at[0, pos[m], at], RT.at[pos[m], at], pts.at[m, p], ptr.at[m, p], peer(1 << k, "B"))

    def iadd(m, p):
        a, n = ip[p]
        v = PI[pos[m] * ROWS + a : pos[m] * ROWS + a + n, :]
        for c in cube.children(p, m):
            imsg(c, p).wait_recv()
            v = v + RI[pos[c] * ROWS + a : pos[c] * ROWS + a + n, :]
        PI[pos[m] * ROWS + a : pos[m] * ROWS + a + n, :] = v

    def oadd(m, p):
        a, n = tp[p]
        v = PT[0, pos[m], a : a + n, :]
        for c in cube.children(p, m):
            omsg(c, p).wait_recv()
            v = v + RT[pos[c], a : a + n, :]
        PT[0, pos[m], a : a + n, :] = v

    going = []

    def ready(m, msg):
        for p in cube.pieces:
            if m and not cube.children(p, m):
                c = msg(m, p)
                c.start()
                going.append(c)

    def follow(level, msg, add):
        todo = [(m, p) for m in order if cube.level[m] == level for p in cube.pieces if cube.children(p, m)]
        todo.sort(key=lambda e: len(cube.children(e[1], e[0])))
        for m, p in todo:
            add(m, p)
            if m:
                c = msg(m, p)
                c.start()
                going.append(c)

    pmsg = {
        m: send(PT.at[1, pos[m]], RTC.at[pos[m]], pcs.at[m], pcr.at[m], peer(0, "B", True)) for m in order
    }

    def pair(m):
        pmsg[m].wait_recv()
        PT[0, pos[m]] = PT[0, pos[m]] + RTC[pos[m]]
        ready(m, omsg)

    far_first = list(reversed(order))
    acc = jnp.zeros((8, 256), jnp.float32)
    behind = []
    with jax.named_scope("texts"):
        for m in far_first:
            cols = slice(pos[m] * 256, (pos[m] + 1) * 256)

            def strip(i, acc, cols=cols):
                at = pl.ds(pl.multiple_of(i * strip_rows, strip_rows), strip_rows)
                v = L[at, cols]
                rl = RREP[at, :]
                w = jnp.exp2(v - jnp.concatenate([rl, rl], axis=1)) + jnp.exp2(v - CROW[:, cols])
                W[at, cols] = w.astype(jnp.bfloat16)
                return acc + jnp.sum((w * v).reshape(strip_rows // 8, 8, 256), axis=0)

            acc = lax.fori_loop(0, rows // strip_rows, strip, acc)
            if m == 0:
                w = jnp.exp2(own - RREP[:128, :]) + jnp.exp2(own - CROW[:, :128])
                W[:128, :128] = (w - eye.astype(jnp.float32)).astype(jnp.bfloat16)
            v = jnp.dot(XT[...], W[:, cols], preferred_element_type=jnp.float32)
            PT[1, pos[m]] = v[:, 128:]
            pmsg[m].start()
            PT[0, pos[m]] = v[:, :128]
            behind.append(m)
            if len(behind) > 2:
                pair(behind.pop(0))

    line = lax.broadcasted_iota(jnp.int32, (8, 128), 0)
    scale_part = LN2 * (jnp.sum(acc) - paired)
    ST[0] = jnp.where(line == 0, loss_part, jnp.where(line == 1, scale_part, 0.0))
    stages = []
    base = 0
    for kind, masks, flip in (("A", range(1, nb), False), ("B", range(1, nb), False), ("B", (0,), True)):
        stages.append((base, [
            send(ST.at[base], ST.at[base + 1 + i], sts.at[base + i], str_.at[base + i], peer(m, kind, flip))
            for i, m in enumerate(masks)
        ]))
        base += 1 + len(masks)

    def stat(i):
        at, copies = stages[i]
        tile = ST[at]
        for j, c in enumerate(copies):
            c.wait_recv()
            tile = tile + ST[at + 1 + j]
        if i + 1 < len(stages):
            ST[stages[i + 1][0]] = tile
            for c in stages[i + 1][1]:
                c.start()
        return tile

    def image_grad(first, last):
        at = slice(first * ROWS, last * ROWS)
        PI[at, :] = jnp.dot(W[at, :], T[...], preferred_element_type=jnp.float32)

    with jax.named_scope("images"):
        for i, lev in enumerate(range(nd, -1, -1)):
            ms = levels[lev]
            image_grad(pos[ms[0]], pos[ms[-1]] + 1)
            for m in ms:
                ready(m, imsg)
            if i == 0:
                for c in stages[0][1]:
                    c.start()
                for m in behind:
                    pair(m)
    with jax.named_scope("follow"):
        for lev in range(nd - 1, 0, -1):
            follow(lev, omsg, oadd)
            follow(lev, imsg, iadd)
            if lev == nd - 1:
                stat(0)
    with jax.named_scope("last"):
        stat(1)
        follow(0, omsg, oadd)
        gt_out[...] = (PT[0, 0] * scale).T.astype(jnp.bfloat16)
        tile = stat(2)
        stats_out[...] = jnp.where(line == 0, tile * (0.5 / total), tile * (1.0 / total))
        follow(0, imsg, iadd)
        gi_out[...] = (PI[:128, :] * scale[:, :1]).astype(jnp.bfloat16)
        for c in going + list(pmsg.values()) + [c for _, cs in stages for c in cs]:
            c.wait_send()


def body(dims, total, images, texts, log_scale):
    nd = len(dims)
    nb = 2**nd
    f32, bf16 = jnp.float32, jnp.bfloat16
    vm, dma = pltpu.VMEM, pltpu.SemaphoreType.DMA
    width = images.shape[1]
    rows, cols = nb * ROWS, 2 * nb * ROWS
    gi, gt, stats = pl.pallas_call(
        functools.partial(kernel, dims, total),
        out_shape=(
            jax.ShapeDtypeStruct(images.shape, bf16),
            jax.ShapeDtypeStruct(texts.shape, bf16),
            jax.ShapeDtypeStruct((8, 128), f32),
        ),
        in_specs=[
            pl.BlockSpec(memory_space=pltpu.SMEM),
            pl.BlockSpec(memory_space=pl.ANY),
            pl.BlockSpec(memory_space=pl.ANY),
        ],
        out_specs=(pl.BlockSpec(memory_space=vm),) * 3,
        scratch_shapes=[
            vm((rows, width), bf16), vm((width, rows), bf16), vm((cols, width), bf16),
            vm((rows, cols), f32), vm((rows, cols), bf16),
            vm((rows, 128), f32), vm((rows, 128), f32), vm((1, cols), f32), vm((1, cols), f32),
            vm((nb, nb, 128), f32), vm((2 * nb, 2 * nb, 128), f32), vm((rows, 128), f32), vm((1, cols), f32),
            vm((rows, width), f32), vm((rows, width), f32),
            vm((2, nb, width, 128), f32), vm((nb, width, 128), f32), vm((nb, width, 128), f32),
            vm((2 * nb + 2, 8, 128), f32),
            dma((2,)), dma((nb, nd)), dma((nb, nd)), dma((nb, nd)), dma((nb, nd)), dma((nb, nd)), dma((nb, nd)),
            dma((nb,)), dma((nb,)), dma((2 * nb,)), dma((2 * nb,)),
            dma((nb, nd)), dma((nb, nd)), dma((nb,)), dma((nb,)), dma((nb, nd)), dma((nb, nd)),
            dma((2 * nb + 2,)), dma((2 * nb + 2,)),
        ],
        compiler_params=pltpu.CompilerParams(
            collective_id=0, has_side_effects=True, vmem_limit_bytes=60 * 2**20
        ),
        name="contrastive",
    )(log_scale.reshape(1), images, texts)
    return gi, gt, stats[0, 0], stats[1, 0]


def solution(mesh):
    return build(Mesh(mesh.devices.reshape(4, 4, 2, 4), AXES))


def build(split):
    dims = tuple(a for a in CUBE if split.shape[a] == 4)
    placed = P(AXES, None)
    return jax.shard_map(
        functools.partial(body, dims, ROWS * split.size),
        mesh=split,
        in_specs=(placed, placed, P()),
        out_specs=(placed, placed, P(), P()),
        check_vma=False,
    )
```

```python
import functools
import math

import jax
import jax.numpy as jnp
from jax import lax
from jax.experimental import pallas as pl
from jax.experimental.pallas import tpu as pltpu
from jax.sharding import Mesh
from jax.sharding import PartitionSpec as P

AXES = ("x", "y", "core", "z")
CUBE = ("x", "y", "z")
MESH = pl.DeviceIdType.MESH
ROWS = 128
LOG2E = math.log2(math.e)
LN2 = math.log(2.0)
NT = (((1,), (1,)), ((), ()))


class Cube:
    def __init__(self, n):
        self.n = n
        self.order = sorted(range(2**n), key=lambda m: (bin(m).count("1"), m))
        self.pos = {m: i for i, m in enumerate(self.order)}
        self.level = {m: bin(m).count("1") for m in self.order}
        self.pieces = range(n)

    def hop(self, p, m):
        return next(k % self.n for k in range(p, p + self.n) if m >> (k % self.n) & 1)

    def children(self, p, m):
        more = [(k, m | 1 << k) for k in range(self.n) if not m >> k & 1]
        return [c for k, c in more if self.hop(p, c) == k]

    def turns(self):
        seen = []
        for q in (1, -1, 0):
            if q % self.n not in seen:
                seen.append(q % self.n)
        return seen


def cut(total, n, unit):
    units = total // unit
    ends = [-(-units * i // n) * unit for i in range(n + 1)]
    return [(a, b - a) for a, b in zip(ends, ends[1:])]


def kernel(
    dims, total,
    log_scale, images, texts,
    gi_out, gt_out, stats_out,
    X, XT, T, L, W, RM, RN, RS, CM, CN, CS, RL, CL, RREP, CROW,
    PI, RI, PT, RTC, RT, ST,
    local_sem, xs, xr, ts, tr, ds, dr, rls, rlr, cls, clr, pis, pir, pcs, pcr, pts, ptr, sts, str_,
):
    nd = len(dims)
    nb = 2**nd
    rows = nb * ROWS
    cube = Cube(nd)
    order, pos = cube.order, cube.pos
    me = {a: lax.axis_index(a) for a in AXES}
    core = me["core"]

    def peer(mask, kind, flip=False):
        ident = {}
        for d, a in enumerate(dims):
            if mask >> d & 1:
                c = me[a]
                ident[a] = c + 1 - 2 * (c % 2) if kind == "A" else 3 - c
        if flip:
            ident["core"] = 1 - core
        return ident

    def spot(mask, kind):
        at = 0
        for d, a in enumerate(dims):
            bit = me[a] % 2 if kind == "A" else me[a] // 2
            at = at + 2**d * (1 - bit if mask >> d & 1 else bit)
        return at

    def send(src, dst, s, r, where):
        return pltpu.make_async_remote_copy(
            src_ref=src, dst_ref=dst, send_sem=s, recv_sem=r, device_id=where, device_id_type=MESH
        )

    with jax.named_scope("enter"):
        ci = pltpu.make_async_copy(images, X.at[pl.ds(0, ROWS)], local_sem.at[0])
        ct = pltpu.make_async_copy(texts, T.at[pl.ds(0, ROWS)], local_sem.at[1])
        ci.start()
        ct.start()
        barrier = pltpu.get_barrier_semaphore()
        others = [(m, "A", False) for m in range(1, nb)]
        others += [(m, "B", f) for m in range(nb) for f in (False, True) if m or f]
        for o in others:
            pl.semaphore_signal(barrier, inc=1, device_id=peer(*o), device_id_type=MESH)
        RM[...] = jnp.full(RM.shape, -3e38, jnp.float32)
        RS[...] = jnp.zeros(RS.shape, jnp.float32)
        CM[...] = jnp.full(CM.shape, -3e38, jnp.float32)
        CS[...] = jnp.zeros(CS.shape, jnp.float32)
        scale = jnp.exp(jnp.full((1, 128), log_scale[0], jnp.float32))
        scale_two = jnp.concatenate([scale * LOG2E] * 2, axis=1)
        ci.wait()
        ct.wait()
        pl.semaphore_wait(barrier, len(others))

    gp = cut(ROWS, nd, 16)
    started = []

    def go(c):
        c.start()
        started.append(c)

    def xmsg(m, p):
        k = cube.hop(p, m)
        a, n = gp[p]
        src = X.at[pl.ds(pos[m ^ 1 << k] * ROWS + a, n)]
        return send(src, X.at[pl.ds(pos[m] * ROWS + a, n)], xs.at[m, p], xr.at[m, p], peer(1 << k, "A"))

    def tmsg(m, p):
        k = cube.hop(p, m)
        a, n = gp[p]
        src = T.at[pl.ds(pos[m ^ 1 << k] * 2 * ROWS + a, n)]
        return send(src, T.at[pl.ds(pos[m] * 2 * ROWS + a, n)], ts.at[m, p], tr.at[m, p], peer(1 << k, "B"))

    def dmsg(m, p):
        a, n = gp[p]
        at = pos[m] * 2 * ROWS + a
        return send(T.at[pl.ds(at, n)], T.at[pl.ds(at + ROWS, n)], ds.at[m, p], dr.at[m, p], peer(0, "B", True))

    def pass_on(events):
        for m, p in events:
            xmsg(m, p).wait_recv()
        nxt = [(c, p) for m, p in events for c in cube.children(p, m)]
        nxt.sort(key=lambda e: not cube.children(e[1], e[0]))
        for e in nxt:
            go(xmsg(*e))
        for m, p in events:
            tmsg(m, p).wait_recv()
        for e in nxt:
            go(tmsg(*e))
        for e in events:
            go(dmsg(*e))

    def logits(r0, r1, c0, c1):
        for i in range(c0, c1):
            cols = slice(i * 256, (i + 1) * 256)
            v = lax.dot_general(X[r0:r1, :], T[cols, :], NT, preferred_element_type=jnp.float32) * scale_two
            L[r0:r1, cols] = v
            RN[r0:r1, :] = jnp.maximum(RN[r0:r1, :], jnp.maximum(v[:, :128], v[:, 128:]))
            CN[:, cols] = jnp.maximum(CN[:, cols], jnp.max(v, axis=0, keepdims=True))

    def new_tops(r1, c1):
        for r in range(0, r1, 128):
            at = slice(r, r + 128)
            top = jnp.broadcast_to(jnp.max(RN[at, :], axis=1, keepdims=True), (128, 128))
            RS[at, :] = RS[at, :] * jnp.exp2(RM[at, :] - top)
            RM[at, :] = top
            RN[at, :] = top
        cols = slice(0, c1 * 256)
        CS[:, cols] = CS[:, cols] * jnp.exp2(CM[:, cols] - CN[:, cols])
        CM[:, cols] = CN[:, cols]

    def sums(r0, r1, c0, c1):
        def step(i, _):
            cols = pl.ds(pl.multiple_of(i * 256, 256), 256)
            cm = CM[:, cols]
            cs = CS[:, cols]
            for r in range(r0, r1, 64):
                at = slice(r, r + 64)
                v = L[at, cols]
                rm = RM[at, :]
                er = jnp.exp2(v[:, :128] - rm) + jnp.exp2(v[:, 128:] - rm)
                RS[at, :] = RS[at, :] + er
                cs = cs + jnp.sum(jnp.exp2(v - cm).reshape(8, 8, 256), axis=0)
            CS[:, cols] = cs
            return 0

        lax.fori_loop(c0, c1, step, 0)

    def partner_texts(masks):
        for m in masks:
            for p in cube.pieces:
                dmsg(m, p).wait_recv()

    with jax.named_scope("gather"):
        for p in cube.pieces:
            go(dmsg(0, p))
        for q in cube.turns():
            for k in range(nd):
                go(xmsg(1 << k, (k + q) % nd))
                go(tmsg(1 << k, (k + q) % nd))
        groups = [[(1 << k, (k + q) % nd) for k in range(nd)] for q in cube.turns()]
        for g in groups:
            pass_on(g)
        levels = [[m for m in order if cube.level[m] == i] for i in range(nd + 1)]
    RN[...] = RM[...]
    CN[...] = CM[...]
    done = 0
    for lev in range(1, nd + 1):
        before = done
        done = sum(len(levels[i]) for i in range(lev + 1))
        old, new = before * ROWS, done * ROWS
        with jax.named_scope(f"gather{lev}"):
            if 1 < lev < nd:
                events = [(m, p) for m in levels[lev] for p in cube.pieces]
                deep = [e for e in events if cube.children(e[1], e[0])]
                if deep:
                    pass_on(deep)
                pass_on([e for e in events if e not in deep])
            partner_texts((levels[0] if lev == 1 else []) + levels[lev])
        with jax.named_scope(f"logits{lev}"):
            if before:
                logits(old, new, 0, before)
            if lev == nd - 1:
                pass_on([(m, p) for m in levels[nd] for p in cube.pieces])
            logits(0, new, before, done)
        with jax.named_scope(f"sums{lev}"):
            new_tops(new, done)
            if before:
                sums(old, new, 0, before)
            sums(0, new, before, done)

    with jax.named_scope("lse"):
        ccol = CM[...] + jnp.log2(jnp.sum(CS[...], axis=0, keepdims=True))
        for m in order:
            for f in range(2):
                at = (2 * pos[m] + f) * 128
                line = (1 - core if f else core) * nb + spot(m, "B")
                CL[0, pl.ds(line, 1), :] = ccol[:, at : at + 128]
        cc = [
            send(CL.at[0], CL.at[2 * m + f], cls.at[2 * m + f], clr.at[2 * m + f], peer(m, "B", f == 1))
            for m in reversed(order) for f in range(2) if m or f
        ]
        for c in cc:
            c.start()
        for m in order:
            at = slice(pos[m] * 128, (pos[m] + 1) * 128)
            top = jnp.max(RM[at, :].T, axis=0, keepdims=True)
            part = jnp.sum(RS[at, :].T, axis=0, keepdims=True)
            RL[0, pl.ds(spot(m, "A"), 1), :] = top + jnp.log2(part)
        rc = [send(RL.at[0], RL.at[m], rls.at[m], rlr.at[m], peer(m, "A")) for m in reversed(order[1:])]
        for c in rc:
            c.start()
    with jax.named_scope("turn"):
        XT[...] = X[...].T
        for c in started:
            c.wait_send()
    with jax.named_scope("lsewait"):
        for c in cc + rc:
            c.wait_recv()
        for c in cc + rc:
            c.wait_send()

    with jax.named_scope("join"):
        def joined(parts):
            top = functools.reduce(jnp.maximum, parts)
            return top + jnp.log2(functools.reduce(jnp.add, [jnp.exp2(p - top) for p in parts]))

        RL[0] = joined([RL[m] for m in range(nb)])
        CL[0] = joined([CL[m] for m in range(2 * nb)])
        for m in order:
            line = RL[0, pl.ds(spot(m, "A"), 1), :]
            RREP[pos[m] * 128 : (pos[m] + 1) * 128, :] = jnp.broadcast_to(line + 1.0, (128, 128)).T
            for f in range(2):
                at = (2 * pos[m] + f) * 128
                CROW[:, at : at + 128] = CL[0, pl.ds((1 - core if f else core) * nb + spot(m, "B"), 1), :] + 1.0
        eye = lax.broadcasted_iota(jnp.int32, (128, 128), 0) == lax.broadcasted_iota(jnp.int32, (128, 128), 1)
        own = L[:128, :128]
        paired = jnp.sum(jnp.where(eye, own, 0.0))
        loss_part = LN2 * (
            jnp.sum(RL[0, pl.ds(spot(0, "A"), 1), :])
            + jnp.sum(CL[0, pl.ds(core * nb + spot(0, "B"), 1), :])
            - 2.0 * paired
        )

    ip = cut(ROWS, nd, 8)
    tp = cut(XT.shape[0], nd, 8)

    def imsg(m, p):
        k = cube.hop(p, m)
        a, n = ip[p]
        at = pl.ds(pos[m] * ROWS + a, n)
        return send(PI.at[at], RI.at[at], pis.at[m, p], pir.at[m, p], peer(1 << k, "A"))

    def omsg(m, p):
        k = cube.hop(p, m)
        a, n = tp[p]
        at = pl.ds(a, n)
        return send(PT.at[0, pos[m], at], RT.at[pos[m], at], pts.at[m, p], ptr.at[m, p], peer(1 << k, "B"))

    def iadd(m, p):
        a, n = ip[p]
        v = PI[pos[m] * ROWS + a : pos[m] * ROWS + a + n, :]
        for c in cube.children(p, m):
            imsg(c, p).wait_recv()
            v = v + RI[pos[c] * ROWS + a : pos[c] * ROWS + a + n, :]
        PI[pos[m] * ROWS + a : pos[m] * ROWS + a + n, :] = v

    def oadd(m, p):
        a, n = tp[p]
        v = PT[0, pos[m], a : a + n, :]
        for c in cube.children(p, m):
            omsg(c, p).wait_recv()
            v = v + RT[pos[c], a : a + n, :]
        PT[0, pos[m], a : a + n, :] = v

    going = []

    def ready(m, msg):
        for p in cube.pieces:
            if m and not cube.children(p, m):
                c = msg(m, p)
                c.start()
                going.append(c)

    def follow(level):
        todo = [(m, p) for m in order if cube.level[m] == level for p in cube.pieces if cube.children(p, m)]
        for n in sorted({len(cube.children(p, m)) for m, p in todo}):
            for msg, add in ((omsg, oadd), (imsg, iadd)):
                for m, p in todo:
                    if len(cube.children(p, m)) == n:
                        add(m, p)
                        c = msg(m, p)
                        c.start()
                        going.append(c)

    pmsg = {
        m: send(PT.at[1, pos[m]], RTC.at[pos[m]], pcs.at[m], pcr.at[m], peer(0, "B", True)) for m in order
    }

    def pair(m):
        pmsg[m].wait_recv()
        PT[0, pos[m]] = PT[0, pos[m]] + RTC[pos[m]]
        ready(m, omsg)

    def weigh(m, acc):
        cols = slice(pos[m] * 256, (pos[m] + 1) * 256)
        cl = CROW[:, cols]
        for r in range(0, rows, 64):
            at = slice(r, r + 64)
            v = L[at, cols]
            rl = RREP[at, :]
            w = jnp.exp2(v - jnp.concatenate([rl, rl], axis=1)) + jnp.exp2(v - cl)
            acc = acc + jnp.sum((w * v).reshape(8, 8, 256), axis=0)
            if m == 0 and r < 128:
                mark = lax.broadcasted_iota(jnp.int32, (64, 256), 0) + r == lax.broadcasted_iota(jnp.int32, (64, 256), 1)
                w = w - mark.astype(jnp.float32)
            W[at, cols] = w.astype(jnp.bfloat16)
        return acc

    far_first = list(reversed(order))
    behind = []
    with jax.named_scope("weigh"):
        acc = weigh(far_first[0], jnp.zeros((8, 256), jnp.float32))
    with jax.named_scope("texts"):
        for i, m in enumerate(far_first):
            cols = slice(pos[m] * 256, (pos[m] + 1) * 256)
            v = jnp.dot(XT[...], W[:, cols], preferred_element_type=jnp.float32)
            if i + 1 < nb:
                acc = weigh(far_first[i + 1], acc)
            PT[1, pos[m]] = v[:, 128:]
            PT[0, pos[m]] = v[:, :128]
            pmsg[m].start()
            behind.append(m)
            if len(behind) > 3:
                pair(behind.pop(0))

    line = lax.broadcasted_iota(jnp.int32, (8, 128), 0)
    scale_part = LN2 * (jnp.sum(acc) - paired)
    ST[0] = jnp.where(line == 0, loss_part, jnp.where(line == 1, scale_part, 0.0))
    stages = []
    base = 0
    for kind, masks, flip in (("A", range(1, nb), False), ("B", range(1, nb), False), ("B", (0,), True)):
        stages.append((base, [
            send(ST.at[base], ST.at[base + 1 + i], sts.at[base + i], str_.at[base + i], peer(m, kind, flip))
            for i, m in enumerate(masks)
        ]))
        base += 1 + len(masks)

    def stat(i):
        at, copies = stages[i]
        tile = ST[at]
        for j, c in enumerate(copies):
            c.wait_recv()
            tile = tile + ST[at + 1 + j]
        if i + 1 < len(stages):
            ST[stages[i + 1][0]] = tile
            for c in stages[i + 1][1]:
                c.start()
        return tile

    def image_grad(first, last):
        at = slice(first * ROWS, last * ROWS)
        PI[at, :] = jnp.dot(W[at, :], T[...], preferred_element_type=jnp.float32)

    with jax.named_scope("images"):
        for i, lev in enumerate(range(nd, -1, -1)):
            ms = levels[lev]
            image_grad(pos[ms[0]], pos[ms[-1]] + 1)
            for m in ms:
                ready(m, imsg)
            if i == 0:
                for c in stages[0][1]:
                    c.start()
                for m in behind:
                    pair(m)
    with jax.named_scope("follow"):
        for lev in range(nd - 1, 0, -1):
            follow(lev)
            if lev == nd - 1:
                stat(0)
    with jax.named_scope("last"):
        stat(1)
        for p in cube.pieces:
            oadd(0, p)
        gt_out[...] = (PT[0, 0] * scale).T.astype(jnp.bfloat16)
        tile = stat(2)
        stats_out[...] = jnp.where(line == 0, tile * (0.5 / total), tile * (1.0 / total))
        for p in cube.pieces:
            iadd(0, p)
        gi_out[...] = (PI[:128, :] * scale[:, :1]).astype(jnp.bfloat16)
        for c in going + list(pmsg.values()) + [c for _, cs in stages for c in cs]:
            c.wait_send()


def hand_over(gi, gt, stats, gi_out, gt_out, loss_out, scale_out):
    gi_out[...] = gi[...]
    gt_out[...] = gt[...]
    loss_out[...] = stats[0:1, 0:1]
    scale_out[...] = stats[1:2, 0:1]


def body(dims, total, images, texts, log_scale):
    nd = len(dims)
    nb = 2**nd
    f32, bf16 = jnp.float32, jnp.bfloat16
    vm, dma = pltpu.VMEM, pltpu.SemaphoreType.DMA
    width = images.shape[1]
    rows, cols = nb * ROWS, 2 * nb * ROWS
    gi, gt, stats = pl.pallas_call(
        functools.partial(kernel, dims, total),
        out_shape=(
            jax.ShapeDtypeStruct(images.shape, bf16),
            jax.ShapeDtypeStruct(texts.shape, bf16),
            jax.ShapeDtypeStruct((8, 128), f32),
        ),
        in_specs=[
            pl.BlockSpec(memory_space=pltpu.SMEM),
            pl.BlockSpec(memory_space=pl.ANY),
            pl.BlockSpec(memory_space=pl.ANY),
        ],
        out_specs=(pl.BlockSpec(memory_space=vm),) * 3,
        scratch_shapes=[
            vm((rows, width), bf16), vm((width, rows), bf16), vm((cols, width), bf16),
            vm((rows, cols), f32), vm((rows, cols), bf16),
            vm((rows, 128), f32), vm((rows, 128), f32), vm((rows, 128), f32),
            vm((1, cols), f32), vm((1, cols), f32), vm((8, cols), f32),
            vm((nb, nb, 128), f32), vm((2 * nb, 2 * nb, 128), f32), vm((rows, 128), f32), vm((1, cols), f32),
            vm((rows, width), f32), vm((rows, width), f32),
            vm((2, nb, width, 128), f32), vm((nb, width, 128), f32), vm((nb, width, 128), f32),
            vm((2 * nb + 2, 8, 128), f32),
            dma((2,)), dma((nb, nd)), dma((nb, nd)), dma((nb, nd)), dma((nb, nd)), dma((nb, nd)), dma((nb, nd)),
            dma((nb,)), dma((nb,)), dma((2 * nb,)), dma((2 * nb,)),
            dma((nb, nd)), dma((nb, nd)), dma((nb,)), dma((nb,)), dma((nb, nd)), dma((nb, nd)),
            dma((2 * nb + 2,)), dma((2 * nb + 2,)),
        ],
        compiler_params=pltpu.CompilerParams(
            collective_id=0, has_side_effects=True, vmem_limit_bytes=60 * 2**20
        ),
        name="contrastive",
    )(log_scale.reshape(1), images, texts)
    outs = pl.pallas_call(
        hand_over,
        out_shape=(
            jax.ShapeDtypeStruct(images.shape, bf16),
            jax.ShapeDtypeStruct(texts.shape, bf16),
            jax.ShapeDtypeStruct((1, 1), f32),
            jax.ShapeDtypeStruct((1, 1), f32),
        ),
        in_specs=[pl.BlockSpec(memory_space=vm)] * 3,
        out_specs=(pl.BlockSpec(memory_space=vm),) * 4,
        name="outputs",
    )(gi, gt, stats)
    return outs[0], outs[1], outs[2].reshape(()), outs[3].reshape(())


def solution(mesh):
    return build(Mesh(mesh.devices.reshape(4, 4, 2, 4), AXES))


def build(split):
    dims = tuple(a for a in CUBE if split.shape[a] == 4)
    placed = P(AXES, None)
    return jax.shard_map(
        functools.partial(body, dims, ROWS * split.size),
        mesh=split,
        in_specs=(placed, placed, P()),
        out_specs=(placed, placed, P(), P()),
        check_vma=False,
    )
```

```python
import functools
import math

import jax
import jax.numpy as jnp
from jax import lax
from jax.experimental import pallas as pl
from jax.experimental.pallas import tpu as pltpu
from jax.sharding import Mesh
from jax.sharding import PartitionSpec as P

AXES = ("x", "y", "core", "z")
CUBE = ("x", "y", "z")
MESH = pl.DeviceIdType.MESH
ROWS = 128
LOG2E = math.log2(math.e)
LN2 = math.log(2.0)
NT = (((1,), (1,)), ((), ()))


class Cube:
    def __init__(self, n):
        self.n = n
        self.order = sorted(range(2**n), key=lambda m: (bin(m).count("1"), m))
        self.pos = {m: i for i, m in enumerate(self.order)}
        self.level = {m: bin(m).count("1") for m in self.order}
        self.pieces = range(n)

    def hop(self, p, m):
        return next(k % self.n for k in range(p, p + self.n) if m >> (k % self.n) & 1)

    def children(self, p, m):
        more = [(k, m | 1 << k) for k in range(self.n) if not m >> k & 1]
        return [c for k, c in more if self.hop(p, c) == k]

    def turns(self):
        seen = []
        for q in (1, -1, 0):
            if q % self.n not in seen:
                seen.append(q % self.n)
        return seen


def cut(total, n, unit):
    units = total // unit
    ends = [-(-units * i // n) * unit for i in range(n + 1)]
    return [(a, b - a) for a, b in zip(ends, ends[1:])]


def kernel(
    dims, total,
    log_scale, images, texts,
    gi_out, gt_out, stats_out,
    X, XT, T, L, W, RM, RN, RS, UR, CM, CN, CS, UC, RL, CL, RREP, CROW,
    PI, RI, PT, RTC, RT, ST,
    local_sem, xs, xr, ts, tr, ds, dr, rls, rlr, cls, clr, pis, pir, pcs, pcr, pts, ptr, sts, str_,
):
    nd = len(dims)
    nb = 2**nd
    rows = nb * ROWS
    cube = Cube(nd)
    order, pos = cube.order, cube.pos
    me = {a: lax.axis_index(a) for a in AXES}
    core = me["core"]

    def peer(mask, kind, flip=False):
        ident = {}
        for d, a in enumerate(dims):
            if mask >> d & 1:
                c = me[a]
                ident[a] = 3 - c if kind == "A" else c + 1 - 2 * (c % 2)
        if flip:
            ident["core"] = 1 - core
        return ident

    def spot(mask, kind):
        at = 0
        for d, a in enumerate(dims):
            bit = me[a] // 2 if kind == "A" else me[a] % 2
            at = at + 2**d * (1 - bit if mask >> d & 1 else bit)
        return at

    def send(src, dst, s, r, where):
        return pltpu.make_async_remote_copy(
            src_ref=src, dst_ref=dst, send_sem=s, recv_sem=r, device_id=where, device_id_type=MESH
        )

    with jax.named_scope("enter"):
        ci = pltpu.make_async_copy(images, X.at[pl.ds(0, ROWS)], local_sem.at[0])
        ct = pltpu.make_async_copy(texts, T.at[pl.ds(0, ROWS)], local_sem.at[1])
        ci.start()
        ct.start()
        barrier = pltpu.get_barrier_semaphore()
        others = [(1 << k, kind, False) for k in range(nd) for kind in "AB"] + [(0, "B", True)]
        for o in others:
            pl.semaphore_signal(barrier, inc=1, device_id=peer(*o), device_id_type=MESH)
        RM[...] = jnp.full(RM.shape, -3e38, jnp.float32)
        RS[...] = jnp.zeros(RS.shape, jnp.float32)
        CM[...] = jnp.full(CM.shape, -3e38, jnp.float32)
        CS[...] = jnp.zeros(CS.shape, jnp.float32)
        UR[...] = jnp.zeros(UR.shape, jnp.float32)
        UC[...] = jnp.zeros(UC.shape, jnp.float32)
        scale = jnp.exp(jnp.full((1, 128), log_scale[0], jnp.float32))
        scale_two = jnp.concatenate([scale * LOG2E] * 2, axis=1)
        ci.wait()
        ct.wait()
        pl.semaphore_wait(barrier, len(others))

    gp = cut(ROWS, nd, 16)
    started = []

    def go(c):
        c.start()
        started.append(c)

    def xmsg(m, p):
        k = cube.hop(p, m)
        a, n = gp[p]
        src = X.at[pl.ds(pos[m ^ 1 << k] * ROWS + a, n)]
        return send(src, X.at[pl.ds(pos[m] * ROWS + a, n)], xs.at[m, p], xr.at[m, p], peer(1 << k, "A"))

    def tmsg(m, p):
        k = cube.hop(p, m)
        a, n = gp[p]
        src = T.at[pl.ds(pos[m ^ 1 << k] * 2 * ROWS + a, n)]
        return send(src, T.at[pl.ds(pos[m] * 2 * ROWS + a, n)], ts.at[m, p], tr.at[m, p], peer(1 << k, "B"))

    def dmsg(m, p):
        a, n = gp[p]
        at = pos[m] * 2 * ROWS + a
        return send(T.at[pl.ds(at, n)], T.at[pl.ds(at + ROWS, n)], ds.at[m, p], dr.at[m, p], peer(0, "B", True))

    def pass_on(events):
        for m, p in events:
            xmsg(m, p).wait_recv()
        nxt = [(c, p) for m, p in events for c in cube.children(p, m)]
        nxt.sort(key=lambda e: not cube.children(e[1], e[0]))
        for e in nxt:
            go(xmsg(*e))
        for m, p in events:
            tmsg(m, p).wait_recv()
        for e in nxt:
            go(tmsg(*e))
        for e in events:
            go(dmsg(*e))

    def logits(r0, r1, c0, c1):
        for i in range(c0, c1):
            cols = slice(i * 256, (i + 1) * 256)
            v = lax.dot_general(X[r0:r1, :], T[cols, :], NT, preferred_element_type=jnp.float32) * scale_two
            L[r0:r1, cols] = v
            RN[r0:r1, :] = jnp.maximum(RN[r0:r1, :], jnp.maximum(v[:, :128], v[:, 128:]))
            CN[:, cols] = jnp.maximum(CN[:, cols], jnp.max(v, axis=0, keepdims=True))

    def new_tops(r1, c1):
        for r in range(0, r1, 128):
            at = slice(r, r + 128)
            top = jnp.broadcast_to(jnp.max(RN[at, :], axis=1, keepdims=True), (128, 128))
            fall = jnp.exp2(RM[at, :] - top)
            RS[at, :] = RS[at, :] * fall
            UR[at, :] = UR[at, :] * fall
            RM[at, :] = top
            RN[at, :] = top
        cols = slice(0, c1 * 256)
        fall = jnp.exp2(CM[:, cols] - CN[:, cols])
        CS[:, cols] = CS[:, cols] * fall
        UC[:, cols] = UC[:, cols] * fall
        CM[:, cols] = CN[:, cols]

    def sums(r0, r1, c0, c1):
        def step(i, _):
            cols = pl.ds(pl.multiple_of(i * 256, 256), 256)
            cm = CM[:, cols]
            cs = CS[:, cols]
            uc = UC[:, cols]
            for r in range(r0, r1, 64):
                at = slice(r, r + 64)
                v = L[at, cols]
                rm = RM[at, :]
                er0 = jnp.exp2(v[:, :128] - rm)
                er1 = jnp.exp2(v[:, 128:] - rm)
                RS[at, :] = RS[at, :] + (er0 + er1)
                UR[at, :] = UR[at, :] + (er0 * v[:, :128] + er1 * v[:, 128:])
                ec = jnp.exp2(v - cm)
                cs = cs + jnp.sum(ec.reshape(8, 8, 256), axis=0)
                uc = uc + jnp.sum((ec * v).reshape(8, 8, 256), axis=0)
            CS[:, cols] = cs
            UC[:, cols] = uc
            return 0

        lax.fori_loop(c0, c1, step, 0)

    def partner_texts(masks):
        for m in masks:
            for p in cube.pieces:
                dmsg(m, p).wait_recv()

    with jax.named_scope("gather"):
        for p in cube.pieces:
            go(dmsg(0, p))
        for q in cube.turns():
            for k in range(nd):
                go(xmsg(1 << k, (k + q) % nd))
                go(tmsg(1 << k, (k + q) % nd))
        groups = [[(1 << k, (k + q) % nd) for k in range(nd)] for q in cube.turns()]
        for g in groups:
            pass_on(g)
        levels = [[m for m in order if cube.level[m] == i] for i in range(nd + 1)]
    RN[...] = RM[...]
    CN[...] = CM[...]
    done = 0
    for lev in range(1, nd + 1):
        before = done
        done = sum(len(levels[i]) for i in range(lev + 1))
        old, new = before * ROWS, done * ROWS
        with jax.named_scope(f"gather{lev}"):
            if 1 < lev < nd:
                events = [(m, p) for m in levels[lev] for p in cube.pieces]
                deep = [e for e in events if cube.children(e[1], e[0])]
                if deep:
                    pass_on(deep)
                pass_on([e for e in events if e not in deep])
            partner_texts((levels[0] if lev == 1 else []) + levels[lev])
        with jax.named_scope(f"logits{lev}"):
            if before:
                logits(old, new, 0, before)
            logits(0, new, before, done)
        with jax.named_scope(f"sums{lev}"):
            new_tops(new, done)
            if before:
                sums(old, new, 0, before)
            if lev == nd - 1:
                pass_on([(m, p) for m in levels[nd] for p in cube.pieces])
            sums(0, new, before, done)

    with jax.named_scope("lse"):
        ccol = CM[...] + jnp.log2(jnp.sum(CS[...], axis=0, keepdims=True))
        for m in order:
            for f in range(2):
                at = (2 * pos[m] + f) * 128
                line = (1 - core if f else core) * nb + spot(m, "B")
                CL[0, pl.ds(line, 1), :] = ccol[:, at : at + 128]
        cc = [
            send(CL.at[0], CL.at[2 * m + f], cls.at[2 * m + f], clr.at[2 * m + f], peer(m, "B", f == 1))
            for m in reversed(order) for f in range(2) if m or f
        ]
        for c in cc:
            c.start()
        for m in order:
            at = slice(pos[m] * 128, (pos[m] + 1) * 128)
            top = jnp.max(RM[at, :].T, axis=0, keepdims=True)
            part = jnp.sum(RS[at, :].T, axis=0, keepdims=True)
            RL[0, pl.ds(spot(m, "A"), 1), :] = top + jnp.log2(part)
        rc = [send(RL.at[0], RL.at[m], rls.at[m], rlr.at[m], peer(m, "A")) for m in reversed(order[1:])]
        for c in rc:
            c.start()
    with jax.named_scope("turn"):
        XT[...] = X[...].T
        for c in started:
            c.wait_send()
    with jax.named_scope("lsewait"):
        for c in cc + rc:
            c.wait_recv()
        for c in cc + rc:
            c.wait_send()

    with jax.named_scope("join"):
        def joined(parts):
            top = functools.reduce(jnp.maximum, parts)
            return top + jnp.log2(functools.reduce(jnp.add, [jnp.exp2(p - top) for p in parts]))

        RL[0] = joined([RL[m] for m in range(nb)])
        CL[0] = joined([CL[m] for m in range(2 * nb)])
        for m in order:
            line = RL[0, pl.ds(spot(m, "A"), 1), :]
            RREP[pos[m] * 128 : (pos[m] + 1) * 128, :] = jnp.broadcast_to(line + 1.0, (128, 128)).T
            for f in range(2):
                at = (2 * pos[m] + f) * 128
                CROW[:, at : at + 128] = CL[0, pl.ds((1 - core if f else core) * nb + spot(m, "B"), 1), :] + 1.0
        eye = lax.broadcasted_iota(jnp.int32, (128, 128), 0) == lax.broadcasted_iota(jnp.int32, (128, 128), 1)
        paired = jnp.sum(jnp.where(eye, L[:128, :128], 0.0).reshape(16, 8, 128), axis=0)
        line = lax.broadcasted_iota(jnp.int32, (8, 128), 0)
        own = RL[0, pl.ds(spot(0, "A"), 1), :] + CL[0, pl.ds(core * nb + spot(0, "B"), 1), :]
        loss_part = jnp.where(line == 0, own, 0.0) - 2.0 * paired

    ip = cut(ROWS, nd, 8)
    tp = cut(XT.shape[0], nd, 8)

    def imsg(m, p):
        k = cube.hop(p, m)
        a, n = ip[p]
        at = pl.ds(pos[m] * ROWS + a, n)
        return send(PI.at[at], RI.at[at], pis.at[m, p], pir.at[m, p], peer(1 << k, "A"))

    def omsg(m, p):
        k = cube.hop(p, m)
        a, n = tp[p]
        at = pl.ds(a, n)
        return send(PT.at[0, pos[m], at], RT.at[pos[m], at], pts.at[m, p], ptr.at[m, p], peer(1 << k, "B"))

    def iadd(m, p):
        a, n = ip[p]
        v = PI[pos[m] * ROWS + a : pos[m] * ROWS + a + n, :]
        for c in cube.children(p, m):
            imsg(c, p).wait_recv()
            v = v + RI[pos[c] * ROWS + a : pos[c] * ROWS + a + n, :]
        PI[pos[m] * ROWS + a : pos[m] * ROWS + a + n, :] = v

    def oadd(m, p):
        a, n = tp[p]
        v = PT[0, pos[m], a : a + n, :]
        for c in cube.children(p, m):
            omsg(c, p).wait_recv()
            v = v + RT[pos[c], a : a + n, :]
        PT[0, pos[m], a : a + n, :] = v

    going = []

    def ready(m, msg):
        for p in cube.pieces:
            if m and not cube.children(p, m):
                c = msg(m, p)
                c.start()
                going.append(c)

    def follow(level, which):
        todo = [(m, p) for m in order if cube.level[m] == level for p in cube.pieces if cube.children(p, m)]
        for n in sorted({len(cube.children(p, m)) for m, p in todo}):
            for msg, add in [{"o": (omsg, oadd), "i": (imsg, iadd)}[w] for w in which]:
                for m, p in todo:
                    if len(cube.children(p, m)) == n:
                        add(m, p)
                        c = msg(m, p)
                        c.start()
                        going.append(c)

    pmsg = {
        m: send(PT.at[1, pos[m]], RTC.at[pos[m]], pcs.at[m], pcr.at[m], peer(0, "B", True)) for m in order
    }

    def pair(m):
        pmsg[m].wait_recv()
        PT[0, pos[m]] = PT[0, pos[m]] + RTC[pos[m]]
        ready(m, omsg)

    def weigh(r0, r1, c0, c1):
        for c in range(c0, c1):
            cols = slice(c * 256, (c + 1) * 256)
            cl = CROW[:, cols]
            for r in range(r0, r1, 64):
                at = slice(r, r + 64)
                v = L[at, cols]
                rl = RREP[at, :]
                w = jnp.exp2(v - jnp.concatenate([rl, rl], axis=1)) + jnp.exp2(v - cl)
                if c == 0 and r < 128:
                    across = lax.broadcasted_iota(jnp.int32, (64, 256), 1)
                    mark = lax.broadcasted_iota(jnp.int32, (64, 256), 0) + r == across
                    w = w - mark.astype(jnp.float32)
                W[at, cols] = w.astype(jnp.bfloat16)

    def text_grad(m):
        cols = slice(pos[m] * 256, (pos[m] + 1) * 256)
        v = jnp.dot(XT[...], W[:, cols], preferred_element_type=jnp.float32)
        PT[1, pos[m]] = v[:, 128:]
        PT[0, pos[m]] = v[:, :128]
        pmsg[m].start()

    def image_grad(first, last):
        at = slice(first * ROWS, last * ROWS)
        PI[at, :] = jnp.dot(W[at, :], T[...], preferred_element_type=jnp.float32)

    far = [(m, f) for m in range(nb) for f in (False, True) if m or f]
    stages = [
        [send(ST.at[0], ST.at[m], sts.at[m], str_.at[m], peer(m, "A")) for m in range(1, nb)],
        [send(ST.at[nb], ST.at[nb + 1 + i], sts.at[nb + i], str_.at[nb + i], peer(m, "B", f)) for i, (m, f) in enumerate(far)],
    ]

    def stat(at, copies):
        tile = ST[at]
        for j, c in enumerate(copies):
            c.wait_recv()
            tile = tile + ST[at + 1 + j]
        return tile

    with jax.named_scope("scalars"):
        part = -paired
        for r in range(0, rows, 128):
            at = slice(r, r + 128)
            part = part + jnp.sum((UR[at, :] * jnp.exp2(RM[at, :] - RREP[at, :])).reshape(16, 8, 128), axis=0)
        both = UC[...] * jnp.exp2(CM[...] - CROW[...])
        for c in range(0, 2 * rows, 128):
            part = part + both[:, c : c + 128]
        ST[0, :8] = loss_part
        ST[0, 8:] = part
        for c in stages[0]:
            c.start()
    waiting = []
    for lev in range(nd, -1, -1):
        first, last = pos[levels[lev][0]], pos[levels[lev][-1]] + 1
        low = 0 if lev == 1 else first
        with jax.named_scope(f"texts{lev}"):
            if lev:
                weigh(0, last * ROWS, low, last)
            for m in levels[lev]:
                text_grad(m)
                for w in waiting:
                    pair(w)
                waiting = []
            waiting = list(levels[lev])
        if lev == 1:
            with jax.named_scope("stats"):
                ST[nb] = stat(0, stages[0])
                for c in stages[1]:
                    c.start()
        with jax.named_scope(f"images{lev}"):
            if lev > 1:
                weigh(first * ROWS, last * ROWS, 0, first)
            image_grad(first, last)
            if lev == 1 < nd:
                follow(nd - 1, "i")
            for m in levels[lev]:
                ready(m, imsg)
            if lev == 1 < nd:
                follow(nd - 1, "o")
    pair(0)
    with jax.named_scope("follow"):
        for lev in range(nd - 2, 0, -1):
            follow(lev, "oi")
    with jax.named_scope("last"):
        for p in cube.pieces:
            oadd(0, p)
        gt_out[...] = (PT[0, 0] * scale).T.astype(jnp.bfloat16)
        for p in cube.pieces:
            iadd(0, p)
        gi_out[...] = (PI[:128, :] * scale[:, :1]).astype(jnp.bfloat16)
        tile = stat(nb, stages[1])
        loss = jnp.sum(tile[:8]) * (LN2 * 0.5 / total)
        grad_scale = jnp.sum(tile[8:]) * (LN2 / total)
        stats_out[...] = jnp.where(line == 0, loss, grad_scale)
        for c in going + list(pmsg.values()) + stages[0] + stages[1]:
            c.wait_send()


def hand_over(gi, gt, stats, gi_out, gt_out, loss_out, scale_out):
    gi_out[...] = gi[...]
    gt_out[...] = gt[...]
    loss_out[...] = stats[0:1, 0:1]
    scale_out[...] = stats[1:2, 0:1]


def body(dims, total, images, texts, log_scale):
    nd = len(dims)
    nb = 2**nd
    f32, bf16 = jnp.float32, jnp.bfloat16
    vm, dma = pltpu.VMEM, pltpu.SemaphoreType.DMA
    width = images.shape[1]
    rows, cols = nb * ROWS, 2 * nb * ROWS
    gi, gt, stats = pl.pallas_call(
        functools.partial(kernel, dims, total),
        out_shape=(
            jax.ShapeDtypeStruct(images.shape, bf16),
            jax.ShapeDtypeStruct(texts.shape, bf16),
            jax.ShapeDtypeStruct((8, 128), f32),
        ),
        in_specs=[
            pl.BlockSpec(memory_space=pltpu.SMEM),
            pl.BlockSpec(memory_space=pl.ANY),
            pl.BlockSpec(memory_space=pl.ANY),
        ],
        out_specs=(pl.BlockSpec(memory_space=vm),) * 3,
        scratch_shapes=[
            vm((rows, width), bf16), vm((width, rows), bf16), vm((cols, width), bf16),
            vm((rows, cols), f32), vm((rows, cols), bf16),
            vm((rows, 128), f32), vm((rows, 128), f32), vm((rows, 128), f32), vm((rows, 128), f32),
            vm((1, cols), f32), vm((1, cols), f32), vm((8, cols), f32), vm((8, cols), f32),
            vm((nb, nb, 128), f32), vm((2 * nb, 2 * nb, 128), f32), vm((rows, 128), f32), vm((1, cols), f32),
            vm((rows, width), f32), vm((rows, width), f32),
            vm((2, nb, width, 128), f32), vm((nb, width, 128), f32), vm((nb, width, 128), f32),
            vm((3 * nb, 16, 128), f32),
            dma((2,)), dma((nb, nd)), dma((nb, nd)), dma((nb, nd)), dma((nb, nd)), dma((nb, nd)), dma((nb, nd)),
            dma((nb,)), dma((nb,)), dma((2 * nb,)), dma((2 * nb,)),
            dma((nb, nd)), dma((nb, nd)), dma((nb,)), dma((nb,)), dma((nb, nd)), dma((nb, nd)),
            dma((3 * nb,)), dma((3 * nb,)),
        ],
        compiler_params=pltpu.CompilerParams(
            collective_id=0, has_side_effects=True, vmem_limit_bytes=60 * 2**20
        ),
        name="contrastive",
    )(log_scale.reshape(1), images, texts)
    outs = pl.pallas_call(
        hand_over,
        out_shape=(
            jax.ShapeDtypeStruct(images.shape, bf16),
            jax.ShapeDtypeStruct(texts.shape, bf16),
            jax.ShapeDtypeStruct((1, 1), f32),
            jax.ShapeDtypeStruct((1, 1), f32),
        ),
        in_specs=[pl.BlockSpec(memory_space=vm)] * 3,
        out_specs=(pl.BlockSpec(memory_space=vm),) * 4,
        name="outputs",
    )(gi, gt, stats)
    return outs[0], outs[1], outs[2].reshape(()), outs[3].reshape(())


def solution(mesh):
    return build(Mesh(mesh.devices.reshape(4, 4, 2, 4), AXES))


def build(split):
    dims = tuple(a for a in CUBE if split.shape[a] == 4)
    placed = P(AXES, None)
    return jax.shard_map(
        functools.partial(body, dims, ROWS * split.size),
        mesh=split,
        in_specs=(placed, placed, P()),
        out_specs=(placed, placed, P(), P()),
        check_vma=False,
    )
```

```python
import functools
import math

import jax
import jax.numpy as jnp
from jax import lax
from jax.experimental import pallas as pl
from jax.experimental.pallas import tpu as pltpu
from jax.sharding import Mesh
from jax.sharding import PartitionSpec as P

AXES = ("x", "y", "core", "z")
CUBE = ("x", "y", "z")
MESH = pl.DeviceIdType.MESH
ROWS = 128
LOG2E = math.log2(math.e)
LN2 = math.log(2.0)
NT = (((1,), (1,)), ((), ()))


class Cube:
    def __init__(self, n):
        self.n = n
        self.order = sorted(range(2**n), key=lambda m: (bin(m).count("1"), m))
        self.pos = {m: i for i, m in enumerate(self.order)}
        self.level = {m: bin(m).count("1") for m in self.order}
        self.pieces = range(n)

    def hop(self, p, m):
        return next(k % self.n for k in range(p, p + self.n) if m >> (k % self.n) & 1)

    def children(self, p, m):
        more = [(k, m | 1 << k) for k in range(self.n) if not m >> k & 1]
        return [c for k, c in more if self.hop(p, c) == k]

    def turns(self):
        seen = []
        for q in (1, -1, 0):
            if q % self.n not in seen:
                seen.append(q % self.n)
        return seen


def cut(total, n, unit):
    units = total // unit
    ends = [-(-units * i // n) * unit for i in range(n + 1)]
    return [(a, b - a) for a, b in zip(ends, ends[1:])]


def kernel(
    dims, total,
    log_scale, images, texts,
    gi_out, gt_out, stats_out,
    X, XT, T, L, W, RM, RN, RS, UR, CM, CN, CS, UC, RL, CL, RREP, CROW,
    PI, RI, PT, RTC, RT, ST,
    local_sem, xs, xr, ts, tr, ds, dr, rls, rlr, cls, clr, pis, pir, pcs, pcr, pts, ptr, sts, str_,
):
    nd = len(dims)
    nb = 2**nd
    rows = nb * ROWS
    cube = Cube(nd)
    order, pos = cube.order, cube.pos
    me = {a: lax.axis_index(a) for a in AXES}
    core = me["core"]

    def peer(mask, kind, flip=False):
        ident = {}
        for d, a in enumerate(dims):
            if mask >> d & 1:
                c = me[a]
                ident[a] = 3 - c if kind == "A" else c + 1 - 2 * (c % 2)
        if flip:
            ident["core"] = 1 - core
        return ident

    def spot(mask, kind):
        at = 0
        for d, a in enumerate(dims):
            bit = me[a] // 2 if kind == "A" else me[a] % 2
            at = at + 2**d * (1 - bit if mask >> d & 1 else bit)
        return at

    def send(src, dst, s, r, where):
        return pltpu.make_async_remote_copy(
            src_ref=src, dst_ref=dst, send_sem=s, recv_sem=r, device_id=where, device_id_type=MESH
        )

    with jax.named_scope("enter"):
        ci = pltpu.make_async_copy(images, X.at[pl.ds(0, ROWS)], local_sem.at[0])
        ct = pltpu.make_async_copy(texts, T.at[pl.ds(0, ROWS)], local_sem.at[1])
        ci.start()
        ct.start()
        barrier = pltpu.get_barrier_semaphore()
        others = [(1 << k, kind, False) for k in range(nd) for kind in "AB"] + [(0, "B", True)]
        for o in others:
            pl.semaphore_signal(barrier, inc=1, device_id=peer(*o), device_id_type=MESH)
        RM[...] = jnp.full(RM.shape, -3e38, jnp.float32)
        RS[...] = jnp.zeros(RS.shape, jnp.float32)
        CM[...] = jnp.full(CM.shape, -3e38, jnp.float32)
        CS[...] = jnp.zeros(CS.shape, jnp.float32)
        UR[...] = jnp.zeros(UR.shape, jnp.float32)
        scale = jnp.exp(jnp.full((1, 128), log_scale[0], jnp.float32))
        scale_two = jnp.concatenate([scale * LOG2E] * 2, axis=1)
        ci.wait()
        ct.wait()
        pl.semaphore_wait(barrier, len(others))

    gp = cut(ROWS, nd, 16)
    started = []

    def go(c):
        c.start()
        started.append(c)

    def xmsg(m, p):
        k = cube.hop(p, m)
        a, n = gp[p]
        src = X.at[pl.ds(pos[m ^ 1 << k] * ROWS + a, n)]
        return send(src, X.at[pl.ds(pos[m] * ROWS + a, n)], xs.at[m, p], xr.at[m, p], peer(1 << k, "A"))

    def tmsg(m, p):
        k = cube.hop(p, m)
        a, n = gp[p]
        src = T.at[pl.ds(pos[m ^ 1 << k] * 2 * ROWS + a, n)]
        return send(src, T.at[pl.ds(pos[m] * 2 * ROWS + a, n)], ts.at[m, p], tr.at[m, p], peer(1 << k, "B"))

    def dmsg(m, p):
        a, n = gp[p]
        at = pos[m] * 2 * ROWS + a
        return send(T.at[pl.ds(at, n)], T.at[pl.ds(at + ROWS, n)], ds.at[m, p], dr.at[m, p], peer(0, "B", True))

    def pass_on(events):
        for m, p in events:
            xmsg(m, p).wait_recv()
        nxt = [(c, p) for m, p in events for c in cube.children(p, m)]
        nxt.sort(key=lambda e: not cube.children(e[1], e[0]))
        for e in nxt:
            go(xmsg(*e))
        for m, p in events:
            tmsg(m, p).wait_recv()
        for e in nxt:
            go(tmsg(*e))
        for e in events:
            go(dmsg(*e))

    def logits(r0, r1, c0, c1):
        for i in range(c0, c1):
            cols = slice(i * 256, (i + 1) * 256)
            v = lax.dot_general(X[r0:r1, :], T[cols, :], NT, preferred_element_type=jnp.float32) * scale_two
            L[r0:r1, cols] = v
            RN[r0:r1, :] = jnp.maximum(RN[r0:r1, :], jnp.maximum(v[:, :128], v[:, 128:]))
            CN[:, cols] = jnp.maximum(CN[:, cols], jnp.max(v, axis=0, keepdims=True))

    def new_tops(r1, c1):
        for r in range(0, r1, 128):
            at = slice(r, r + 128)
            top = jnp.broadcast_to(jnp.max(RN[at, :], axis=1, keepdims=True), (128, 128))
            RS[at, :] = RS[at, :] * jnp.exp2(RM[at, :] - top)
            RM[at, :] = top
            RN[at, :] = top
        cols = slice(0, c1 * 256)
        CS[:, cols] = CS[:, cols] * jnp.exp2(CM[:, cols] - CN[:, cols])
        CM[:, cols] = CN[:, cols]

    def sums(r0, r1, c0, c1):
        def step(i, _):
            cols = pl.ds(pl.multiple_of(i * 256, 256), 256)
            cm = CM[:, cols]
            cs = CS[:, cols]
            for r in range(r0, r1, 64):
                at = slice(r, r + 64)
                v = L[at, cols]
                rm = RM[at, :]
                er0 = jnp.exp2(v[:, :128] - rm)
                er1 = jnp.exp2(v[:, 128:] - rm)
                RS[at, :] = RS[at, :] + (er0 + er1)
                ec = jnp.exp2(v - cm)
                cs = cs + jnp.sum(ec.reshape(8, 8, 256), axis=0)
            CS[:, cols] = cs
            return 0

        lax.fori_loop(c0, c1, step, 0)

    def partner_texts(masks):
        for m in masks:
            for p in cube.pieces:
                dmsg(m, p).wait_recv()

    with jax.named_scope("gather"):
        for p in cube.pieces:
            go(dmsg(0, p))
        for q in cube.turns():
            for k in range(nd):
                go(xmsg(1 << k, (k + q) % nd))
                go(tmsg(1 << k, (k + q) % nd))
        groups = [[(1 << k, (k + q) % nd) for k in range(nd)] for q in cube.turns()]
        for g in groups:
            pass_on(g)
        levels = [[m for m in order if cube.level[m] == i] for i in range(nd + 1)]
    RN[...] = RM[...]
    CN[...] = CM[...]
    done = 0
    for lev in range(1, nd + 1):
        before = done
        done = sum(len(levels[i]) for i in range(lev + 1))
        old, new = before * ROWS, done * ROWS
        with jax.named_scope(f"gather{lev}"):
            if 1 < lev < nd:
                events = [(m, p) for m in levels[lev] for p in cube.pieces]
                deep = [e for e in events if cube.children(e[1], e[0])]
                if deep:
                    pass_on(deep)
                pass_on([e for e in events if e not in deep])
            partner_texts((levels[0] if lev == 1 else []) + levels[lev])
        with jax.named_scope(f"logits{lev}"):
            if before:
                logits(old, new, 0, before)
            logits(0, new, before, done)
        with jax.named_scope(f"sums{lev}"):
            new_tops(new, done)
            if before:
                sums(old, new, 0, before)
            if lev == nd - 1:
                pass_on([(m, p) for m in levels[nd] for p in cube.pieces])
            sums(0, new, before, done)

    with jax.named_scope("lse"):
        ccol = CM[...] + jnp.log2(jnp.sum(CS[...], axis=0, keepdims=True))
        for m in order:
            for f in range(2):
                at = (2 * pos[m] + f) * 128
                line = (1 - core if f else core) * nb + spot(m, "B")
                CL[0, pl.ds(line, 1), :] = ccol[:, at : at + 128]
        cc = [
            send(CL.at[0], CL.at[2 * m + f], cls.at[2 * m + f], clr.at[2 * m + f], peer(m, "B", f == 1))
            for m in reversed(order) for f in range(2) if m or f
        ]
        for c in cc:
            c.start()
        for m in order:
            at = slice(pos[m] * 128, (pos[m] + 1) * 128)
            top = jnp.max(RM[at, :].T, axis=0, keepdims=True)
            part = jnp.sum(RS[at, :].T, axis=0, keepdims=True)
            RL[0, pl.ds(spot(m, "A"), 1), :] = top + jnp.log2(part)
        rc = [send(RL.at[0], RL.at[m], rls.at[m], rlr.at[m], peer(m, "A")) for m in reversed(order[1:])]
        for c in rc:
            c.start()
    with jax.named_scope("turn"):
        def tilt(c, _):
            cols = pl.ds(pl.multiple_of(c * 256, 256), 256)
            cm = CM[:, cols]

            def strip(i, uc):
                at = pl.ds(pl.multiple_of(i * 256, 256), 256)
                v = L[at, cols]
                rm = RM[at, :]
                v0, v1 = v[:, :128], v[:, 128:]
                UR[at, :] = UR[at, :] + (jnp.exp2(v0 - rm) * v0 + jnp.exp2(v1 - rm) * v1)
                return uc + jnp.sum((jnp.exp2(v - cm) * v).reshape(32, 8, 256), axis=0)

            UC[:, cols] = lax.fori_loop(0, rows // 256, strip, jnp.zeros((8, 256), jnp.float32))
            return 0

        lax.fori_loop(0, nb, tilt, 0)
        XT[...] = X[...].T
        for c in started:
            c.wait_send()
    with jax.named_scope("lsewait"):
        for c in cc + rc:
            c.wait_recv()
        for c in cc + rc:
            c.wait_send()

    with jax.named_scope("join"):
        def joined(parts):
            top = functools.reduce(jnp.maximum, parts)
            return top + jnp.log2(functools.reduce(jnp.add, [jnp.exp2(p - top) for p in parts]))

        RL[0] = joined([RL[m] for m in range(nb)])
        CL[0] = joined([CL[m] for m in range(2 * nb)])
        for m in order:
            line = RL[0, pl.ds(spot(m, "A"), 1), :]
            RREP[pos[m] * 128 : (pos[m] + 1) * 128, :] = jnp.broadcast_to(line + 1.0, (128, 128)).T
            for f in range(2):
                at = (2 * pos[m] + f) * 128
                CROW[:, at : at + 128] = CL[0, pl.ds((1 - core if f else core) * nb + spot(m, "B"), 1), :] + 1.0
        eye = lax.broadcasted_iota(jnp.int32, (128, 128), 0) == lax.broadcasted_iota(jnp.int32, (128, 128), 1)
        paired = jnp.sum(jnp.where(eye, L[:128, :128], 0.0).reshape(16, 8, 128), axis=0)
        line = lax.broadcasted_iota(jnp.int32, (8, 128), 0)
        own = RL[0, pl.ds(spot(0, "A"), 1), :] + CL[0, pl.ds(core * nb + spot(0, "B"), 1), :]
        loss_part = jnp.where(line == 0, own, 0.0) - 2.0 * paired

    ip = cut(ROWS, nd, 8)
    tp = cut(XT.shape[0], nd, 8)

    def imsg(m, p):
        k = cube.hop(p, m)
        a, n = ip[p]
        at = pl.ds(pos[m] * ROWS + a, n)
        return send(PI.at[at], RI.at[at], pis.at[m, p], pir.at[m, p], peer(1 << k, "A"))

    def omsg(m, p):
        k = cube.hop(p, m)
        a, n = tp[p]
        at = pl.ds(a, n)
        return send(PT.at[0, pos[m], at], RT.at[pos[m], at], pts.at[m, p], ptr.at[m, p], peer(1 << k, "B"))

    def iadd(m, p):
        a, n = ip[p]
        v = PI[pos[m] * ROWS + a : pos[m] * ROWS + a + n, :]
        for c in cube.children(p, m):
            imsg(c, p).wait_recv()
            v = v + RI[pos[c] * ROWS + a : pos[c] * ROWS + a + n, :]
        PI[pos[m] * ROWS + a : pos[m] * ROWS + a + n, :] = v

    def oadd(m, p):
        a, n = tp[p]
        v = PT[0, pos[m], a : a + n, :]
        for c in cube.children(p, m):
            omsg(c, p).wait_recv()
            v = v + RT[pos[c], a : a + n, :]
        PT[0, pos[m], a : a + n, :] = v

    going = []

    def ready(m, msg):
        for p in cube.pieces:
            if m and not cube.children(p, m):
                c = msg(m, p)
                c.start()
                going.append(c)

    def follow(level, which):
        todo = [(m, p) for m in order if cube.level[m] == level for p in cube.pieces if cube.children(p, m)]
        for n in sorted({len(cube.children(p, m)) for m, p in todo}):
            for msg, add in [{"o": (omsg, oadd), "i": (imsg, iadd)}[w] for w in which]:
                for m, p in todo:
                    if len(cube.children(p, m)) == n:
                        add(m, p)
                        c = msg(m, p)
                        c.start()
                        going.append(c)

    pmsg = {
        m: send(PT.at[1, pos[m]], RTC.at[pos[m]], pcs.at[m], pcr.at[m], peer(0, "B", True)) for m in order
    }

    def pair(m):
        pmsg[m].wait_recv()
        PT[0, pos[m]] = PT[0, pos[m]] + RTC[pos[m]]
        ready(m, omsg)

    def weigh(r0, r1, c0, c1):
        for c in range(c0, c1):
            cols = slice(c * 256, (c + 1) * 256)
            cl = CROW[:, cols]
            for r in range(r0, r1, 64):
                at = slice(r, r + 64)
                v = L[at, cols]
                rl = RREP[at, :]
                w = jnp.exp2(v - jnp.concatenate([rl, rl], axis=1)) + jnp.exp2(v - cl)
                if c == 0 and r < 128:
                    across = lax.broadcasted_iota(jnp.int32, (64, 256), 1)
                    mark = lax.broadcasted_iota(jnp.int32, (64, 256), 0) + r == across
                    w = w - mark.astype(jnp.float32)
                W[at, cols] = w.astype(jnp.bfloat16)

    def text_grad(m):
        cols = slice(pos[m] * 256, (pos[m] + 1) * 256)
        v = jnp.dot(XT[...], W[:, cols], preferred_element_type=jnp.float32)
        PT[1, pos[m]] = v[:, 128:]
        PT[0, pos[m]] = v[:, :128]
        pmsg[m].start()

    def image_grad(first, last):
        at = slice(first * ROWS, last * ROWS)
        PI[at, :] = jnp.dot(W[at, :], T[...], preferred_element_type=jnp.float32)

    far = [(m, f) for m in range(nb) for f in (False, True) if m or f]
    stages = [
        [send(ST.at[0], ST.at[m], sts.at[m], str_.at[m], peer(m, "A")) for m in range(1, nb)],
        [send(ST.at[nb], ST.at[nb + 1 + i], sts.at[nb + i], str_.at[nb + i], peer(m, "B", f)) for i, (m, f) in enumerate(far)],
    ]

    def stat(at, copies):
        tile = ST[at]
        for j, c in enumerate(copies):
            c.wait_recv()
            tile = tile + ST[at + 1 + j]
        return tile

    with jax.named_scope("scalars"):
        part = -paired
        for r in range(0, rows, 128):
            at = slice(r, r + 128)
            part = part + jnp.sum((UR[at, :] * jnp.exp2(RM[at, :] - RREP[at, :])).reshape(16, 8, 128), axis=0)
        both = UC[...] * jnp.exp2(CM[...] - CROW[...])
        for c in range(0, 2 * rows, 128):
            part = part + both[:, c : c + 128]
        ST[0, :8] = loss_part
        ST[0, 8:] = part
        for c in stages[0]:
            c.start()
    waiting = []
    for lev in range(nd, -1, -1):
        first, last = pos[levels[lev][0]], pos[levels[lev][-1]] + 1
        low = 0 if lev == 1 else first
        with jax.named_scope(f"texts{lev}"):
            if lev:
                weigh(0, last * ROWS, low, last)
            for m in levels[lev]:
                text_grad(m)
                for w in waiting:
                    pair(w)
                waiting = []
        if lev == 1:
            with jax.named_scope("stats"):
                ST[nb] = stat(0, stages[0])
                for c in stages[1]:
                    c.start()
        with jax.named_scope(f"images{lev}"):
            if lev > 1:
                weigh(first * ROWS, last * ROWS, 0, first)
            image_grad(first, last)
            if lev == 1 < nd:
                follow(nd - 1, "i")
            for m in levels[lev]:
                ready(m, imsg)
            if lev == 1 < nd:
                follow(nd - 1, "o")
            if lev == nd:
                waiting = list(levels[lev])
            else:
                for m in levels[lev]:
                    pair(m)
    with jax.named_scope("follow"):
        for lev in range(nd - 2, 0, -1):
            follow(lev, "oi")
    with jax.named_scope("last"):
        for p in cube.pieces:
            oadd(0, p)
        gt_out[...] = (PT[0, 0] * scale).T.astype(jnp.bfloat16)
        for p in cube.pieces:
            iadd(0, p)
        gi_out[...] = (PI[:128, :] * scale[:, :1]).astype(jnp.bfloat16)
        tile = stat(nb, stages[1])
        loss = jnp.sum(tile[:8]) * (LN2 * 0.5 / total)
        grad_scale = jnp.sum(tile[8:]) * (LN2 / total)
        stats_out[...] = jnp.where(line == 0, loss, grad_scale)
        for c in going + list(pmsg.values()) + stages[0] + stages[1]:
            c.wait_send()


def hand_over(gi, gt, stats, gi_out, gt_out, loss_out, scale_out):
    gi_out[...] = gi[...]
    gt_out[...] = gt[...]
    loss_out[...] = stats[0:1, 0:1]
    scale_out[...] = stats[1:2, 0:1]


def body(dims, total, images, texts, log_scale):
    nd = len(dims)
    nb = 2**nd
    f32, bf16 = jnp.float32, jnp.bfloat16
    vm, dma = pltpu.VMEM, pltpu.SemaphoreType.DMA
    width = images.shape[1]
    rows, cols = nb * ROWS, 2 * nb * ROWS
    gi, gt, stats = pl.pallas_call(
        functools.partial(kernel, dims, total),
        out_shape=(
            jax.ShapeDtypeStruct(images.shape, bf16),
            jax.ShapeDtypeStruct(texts.shape, bf16),
            jax.ShapeDtypeStruct((8, 128), f32),
        ),
        in_specs=[
            pl.BlockSpec(memory_space=pltpu.SMEM),
            pl.BlockSpec(memory_space=pl.ANY),
            pl.BlockSpec(memory_space=pl.ANY),
        ],
        out_specs=(pl.BlockSpec(memory_space=vm),) * 3,
        scratch_shapes=[
            vm((rows, width), bf16), vm((width, rows), bf16), vm((cols, width), bf16),
            vm((rows, cols), f32), vm((rows, cols), bf16),
            vm((rows, 128), f32), vm((rows, 128), f32), vm((rows, 128), f32), vm((rows, 128), f32),
            vm((1, cols), f32), vm((1, cols), f32), vm((8, cols), f32), vm((8, cols), f32),
            vm((nb, nb, 128), f32), vm((2 * nb, 2 * nb, 128), f32), vm((rows, 128), f32), vm((1, cols), f32),
            vm((rows, width), f32), vm((rows, width), f32),
            vm((2, nb, width, 128), f32), vm((nb, width, 128), f32), vm((nb, width, 128), f32),
            vm((3 * nb, 16, 128), f32),
            dma((2,)), dma((nb, nd)), dma((nb, nd)), dma((nb, nd)), dma((nb, nd)), dma((nb, nd)), dma((nb, nd)),
            dma((nb,)), dma((nb,)), dma((2 * nb,)), dma((2 * nb,)),
            dma((nb, nd)), dma((nb, nd)), dma((nb,)), dma((nb,)), dma((nb, nd)), dma((nb, nd)),
            dma((3 * nb,)), dma((3 * nb,)),
        ],
        compiler_params=pltpu.CompilerParams(
            collective_id=0, has_side_effects=True, vmem_limit_bytes=60 * 2**20
        ),
        name="contrastive",
    )(log_scale.reshape(1), images, texts)
    outs = pl.pallas_call(
        hand_over,
        out_shape=(
            jax.ShapeDtypeStruct(images.shape, bf16),
            jax.ShapeDtypeStruct(texts.shape, bf16),
            jax.ShapeDtypeStruct((1, 1), f32),
            jax.ShapeDtypeStruct((1, 1), f32),
        ),
        in_specs=[pl.BlockSpec(memory_space=vm)] * 3,
        out_specs=(pl.BlockSpec(memory_space=vm),) * 4,
        name="outputs",
    )(gi, gt, stats)
    return outs[0], outs[1], outs[2].reshape(()), outs[3].reshape(())


def solution(mesh):
    return build(Mesh(mesh.devices.reshape(4, 4, 2, 4), AXES))


def build(split):
    dims = tuple(a for a in CUBE if split.shape[a] == 4)
    placed = P(AXES, None)
    return jax.shard_map(
        functools.partial(body, dims, ROWS * split.size),
        mesh=split,
        in_specs=(placed, placed, P()),
        out_specs=(placed, placed, P(), P()),
        check_vma=False,
    )
```

```python
import functools
import math

import jax
import jax.numpy as jnp
from jax import lax
from jax.experimental import pallas as pl
from jax.experimental.pallas import tpu as pltpu
from jax.sharding import Mesh
from jax.sharding import PartitionSpec as P

AXES = ("x", "y", "core", "z")
CUBE = ("x", "y", "z")
MESH = pl.DeviceIdType.MESH
ROWS = 128
LOG2E = math.log2(math.e)
LN2 = math.log(2.0)
NT = (((1,), (1,)), ((), ()))


class Cube:
    def __init__(self, n):
        self.n = n
        self.order = sorted(range(2**n), key=lambda m: (bin(m).count("1"), m))
        self.pos = {m: i for i, m in enumerate(self.order)}
        self.level = {m: bin(m).count("1") for m in self.order}
        self.pieces = range(n)

    def hop(self, p, m):
        return next(k % self.n for k in range(p, p + self.n) if m >> (k % self.n) & 1)

    def children(self, p, m):
        more = [(k, m | 1 << k) for k in range(self.n) if not m >> k & 1]
        return [c for k, c in more if self.hop(p, c) == k]

    def turns(self):
        seen = []
        for q in (1, -1, 0):
            if q % self.n not in seen:
                seen.append(q % self.n)
        return seen


def cut(total, n, unit):
    units = total // unit
    ends = [-(-units * i // n) * unit for i in range(n + 1)]
    return [(a, b - a) for a, b in zip(ends, ends[1:])]


def kernel(
    dims, total,
    log_scale, images, texts,
    gi_out, gt_out, stats_out,
    X, XT, T, L, W, RM, RN, RS, UR, CM, CN, CS, UC, RL, CL, RREP, CROW,
    PI, RI, PT, RTC, RT, ST,
    local_sem, xs, xr, ts, tr, ds, dr, rls, rlr, cls, clr, pis, pir, pcs, pcr, pts, ptr, sts, str_,
):
    nd = len(dims)
    nb = 2**nd
    rows = nb * ROWS
    cube = Cube(nd)
    order, pos = cube.order, cube.pos
    me = {a: lax.axis_index(a) for a in AXES}
    core = me["core"]

    def peer(mask, kind, flip=False):
        ident = {}
        for d, a in enumerate(dims):
            if mask >> d & 1:
                c = me[a]
                ident[a] = 3 - c if kind == "A" else c + 1 - 2 * (c % 2)
        if flip:
            ident["core"] = 1 - core
        return ident

    def spot(mask, kind):
        at = 0
        for d, a in enumerate(dims):
            bit = me[a] // 2 if kind == "A" else me[a] % 2
            at = at + 2**d * (1 - bit if mask >> d & 1 else bit)
        return at

    def send(src, dst, s, r, where):
        return pltpu.make_async_remote_copy(
            src_ref=src, dst_ref=dst, send_sem=s, recv_sem=r, device_id=where, device_id_type=MESH
        )

    with jax.named_scope("enter"):
        ci = pltpu.make_async_copy(images, X.at[pl.ds(0, ROWS)], local_sem.at[0])
        ct = pltpu.make_async_copy(texts, T.at[pl.ds(0, ROWS)], local_sem.at[1])
        ci.start()
        ct.start()
        barrier = pltpu.get_barrier_semaphore()
        others = [(1 << k, kind, False) for k in range(nd) for kind in "AB"] + [(0, "B", True)]
        for o in others:
            pl.semaphore_signal(barrier, inc=1, device_id=peer(*o), device_id_type=MESH)
        RM[...] = jnp.full(RM.shape, -3e38, jnp.float32)
        RS[...] = jnp.zeros(RS.shape, jnp.float32)
        CM[...] = jnp.full(CM.shape, -3e38, jnp.float32)
        CS[...] = jnp.zeros(CS.shape, jnp.float32)
        UR[...] = jnp.zeros(UR.shape, jnp.float32)
        scale = jnp.exp(jnp.full((1, 128), log_scale[()], jnp.float32))
        scale_two = jnp.concatenate([scale * LOG2E] * 2, axis=1)
        ci.wait()
        ct.wait()
        pl.semaphore_wait(barrier, len(others))

    gp = cut(ROWS, nd, 16)
    started = []

    def go(c):
        c.start()
        started.append(c)

    def xmsg(m, p):
        k = cube.hop(p, m)
        a, n = gp[p]
        src = X.at[pl.ds(pos[m ^ 1 << k] * ROWS + a, n)]
        return send(src, X.at[pl.ds(pos[m] * ROWS + a, n)], xs.at[m, p], xr.at[m, p], peer(1 << k, "A"))

    def tmsg(m, p):
        k = cube.hop(p, m)
        a, n = gp[p]
        src = T.at[pl.ds(pos[m ^ 1 << k] * 2 * ROWS + a, n)]
        return send(src, T.at[pl.ds(pos[m] * 2 * ROWS + a, n)], ts.at[m, p], tr.at[m, p], peer(1 << k, "B"))

    def dmsg(m, p):
        a, n = gp[p]
        at = pos[m] * 2 * ROWS + a
        return send(T.at[pl.ds(at, n)], T.at[pl.ds(at + ROWS, n)], ds.at[m, p], dr.at[m, p], peer(0, "B", True))

    def pass_on(events):
        for m, p in events:
            xmsg(m, p).wait_recv()
        nxt = [(c, p) for m, p in events for c in cube.children(p, m)]
        nxt.sort(key=lambda e: not cube.children(e[1], e[0]))
        for e in nxt:
            go(xmsg(*e))
        for m, p in events:
            tmsg(m, p).wait_recv()
        for e in nxt:
            go(tmsg(*e))
        for e in events:
            go(dmsg(*e))

    def logits(r0, r1, c0, c1):
        for i in range(c0, c1):
            cols = slice(i * 256, (i + 1) * 256)
            v = lax.dot_general(X[r0:r1, :], T[cols, :], NT, preferred_element_type=jnp.float32) * scale_two
            L[r0:r1, cols] = v
            RN[r0:r1, :] = jnp.maximum(RN[r0:r1, :], jnp.maximum(v[:, :128], v[:, 128:]))
            CN[:, cols] = jnp.maximum(CN[:, cols], jnp.max(v.reshape(-1, 8, 256), axis=0))

    def new_tops(r0, r1, c0, c1):
        at = slice(r0, r1)
        RS[at, :] = RS[at, :] * jnp.exp2(RM[at, :] - RN[at, :])
        RM[at, :] = RN[at, :]
        cols = slice(c0 * 256, c1 * 256)
        CS[:, cols] = CS[:, cols] * jnp.exp2(CM[:, cols] - CN[:, cols])
        CM[:, cols] = CN[:, cols]

    def sums(r0, r1, c0, c1):
        def step(i, _):
            cols = pl.ds(pl.multiple_of(i * 256, 256), 256)
            cm = CM[:, cols]
            cs = CS[:, cols]
            for r in range(r0, r1, 64):
                at = slice(r, r + 64)
                v = L[at, cols]
                rm = RM[at, :]
                er0 = jnp.exp2(v[:, :128] - rm)
                er1 = jnp.exp2(v[:, 128:] - rm)
                RS[at, :] = RS[at, :] + (er0 + er1)
                ec = jnp.exp2(v.reshape(8, 8, 256) - cm)
                cs = cs + jnp.sum(ec, axis=0)
            CS[:, cols] = cs
            return 0

        lax.fori_loop(c0, c1, step, 0)

    def partner_texts(masks):
        for m in masks:
            for p in cube.pieces:
                dmsg(m, p).wait_recv()

    with jax.named_scope("gather"):
        for p in cube.pieces:
            go(dmsg(0, p))
        for q in cube.turns():
            for k in range(nd):
                go(xmsg(1 << k, (k + q) % nd))
                go(tmsg(1 << k, (k + q) % nd))
        levels = [[m for m in order if cube.level[m] == i] for i in range(nd + 1)]
        RN[...] = RM[...]
        CN[...] = CM[...]
        partner_texts(levels[0])
        logits(0, ROWS, 0, 1)
        new_tops(0, ROWS, 0, 1)
        sums(0, ROWS, 0, 1)
        groups = [[(1 << k, (k + q) % nd) for k in range(nd)] for q in cube.turns()]
        for g in groups:
            pass_on(g)
    for lev in range(1, nd + 1):
        before = sum(len(levels[i]) for i in range(lev))
        done = before + len(levels[lev])
        old, new = before * ROWS, done * ROWS
        with jax.named_scope(f"gather{lev}"):
            if 1 < lev < nd:
                events = [(m, p) for m in levels[lev] for p in cube.pieces]
                deep = [e for e in events if cube.children(e[1], e[0])]
                if deep:
                    pass_on(deep)
                pass_on([e for e in events if e not in deep])
            elif lev > 1:
                pass_on([(m, p) for m in levels[lev] for p in cube.pieces])
        with jax.named_scope(f"rows{lev}"):
            logits(old, new, 0, before)
            new_tops(old, new, 0, before)
            sums(old, new, 0, before)
        with jax.named_scope(f"partner{lev}"):
            partner_texts(levels[lev])
        with jax.named_scope(f"columns{lev}"):
            logits(0, new, before, done)
            new_tops(0, new, before, done)
            sums(0, new, before, done)

    with jax.named_scope("lse"):
        ctop = jnp.max(CM[...], axis=0, keepdims=True)
        ccol = ctop + jnp.log2(jnp.sum(CS[...] * jnp.exp2(CM[...] - ctop), axis=0, keepdims=True))
        for m in order:
            for f in range(2):
                at = (2 * pos[m] + f) * 128
                line = (1 - core if f else core) * nb + spot(m, "B")
                CL[0, pl.ds(line, 1), :] = ccol[:, at : at + 128]
        cc = [
            send(CL.at[0], CL.at[2 * m + f], cls.at[2 * m + f], clr.at[2 * m + f], peer(m, "B", f == 1))
            for m in reversed(order) for f in range(2) if m or f
        ]
        for c in cc:
            c.start()
        for m in order:
            at = slice(pos[m] * 128, (pos[m] + 1) * 128)
            tops = RM[at, :].T
            top = jnp.max(tops, axis=0, keepdims=True)
            part = jnp.sum(RS[at, :].T * jnp.exp2(tops - top), axis=0, keepdims=True)
            RL[0, pl.ds(spot(m, "A"), 1), :] = top + jnp.log2(part)
        rc = [send(RL.at[0], RL.at[m], rls.at[m], rlr.at[m], peer(m, "A")) for m in reversed(order[1:])]
        for c in rc:
            c.start()
    with jax.named_scope("turn"):
        def tilt(c, _):
            cols = pl.ds(pl.multiple_of(c * 256, 256), 256)
            cm = CM[:, cols]

            def strip(i, uc):
                at = pl.ds(pl.multiple_of(i * 256, 256), 256)
                v = L[at, cols]
                rm = RM[at, :]
                v0, v1 = v[:, :128], v[:, 128:]
                UR[at, :] = UR[at, :] + (jnp.exp2(v0 - rm) * v0 + jnp.exp2(v1 - rm) * v1)
                w = v.reshape(32, 8, 256)
                return uc + jnp.sum(jnp.exp2(w - cm) * w, axis=0)

            UC[:, cols] = lax.fori_loop(0, rows // 256, strip, jnp.zeros((8, 256), jnp.float32))
            return 0

        lax.fori_loop(0, nb, tilt, 0)
        XT[...] = X[...].T
        for c in started:
            c.wait_send()
    with jax.named_scope("lsewait"):
        for c in cc + rc:
            c.wait_recv()
        for c in cc + rc:
            c.wait_send()

    with jax.named_scope("join"):
        def joined(parts):
            top = functools.reduce(jnp.maximum, parts)
            return top + jnp.log2(functools.reduce(jnp.add, [jnp.exp2(p - top) for p in parts]))

        RL[0] = joined([RL[m] for m in range(nb)])
        CL[0] = joined([CL[m] for m in range(2 * nb)])
        for m in order:
            line = RL[0, pl.ds(spot(m, "A"), 1), :]
            RREP[pos[m] * 128 : (pos[m] + 1) * 128, :] = jnp.broadcast_to(line + 1.0, (128, 128)).T
            for f in range(2):
                at = (2 * pos[m] + f) * 128
                CROW[:, at : at + 128] = CL[0, pl.ds((1 - core if f else core) * nb + spot(m, "B"), 1), :] + 1.0
        eye = lax.broadcasted_iota(jnp.int32, (128, 128), 0) == lax.broadcasted_iota(jnp.int32, (128, 128), 1)
        paired = jnp.sum(jnp.where(eye, L[:128, :128], 0.0).reshape(16, 8, 128), axis=0)
        line = lax.broadcasted_iota(jnp.int32, (8, 128), 0)
        own = RL[0, pl.ds(spot(0, "A"), 1), :] + CL[0, pl.ds(core * nb + spot(0, "B"), 1), :]
        loss_part = jnp.where(line == 0, own, 0.0) - 2.0 * paired

    ip = cut(ROWS, nd, 8)
    tp = cut(XT.shape[0], nd, 8)

    def imsg(m, p):
        k = cube.hop(p, m)
        a, n = ip[p]
        at = pl.ds(pos[m] * ROWS + a, n)
        return send(PI.at[at], RI.at[at], pis.at[m, p], pir.at[m, p], peer(1 << k, "A"))

    def omsg(m, p):
        k = cube.hop(p, m)
        a, n = tp[p]
        at = pl.ds(a, n)
        return send(PT.at[0, pos[m], at], RT.at[pos[m], at], pts.at[m, p], ptr.at[m, p], peer(1 << k, "B"))

    def iadd(m, p):
        a, n = ip[p]
        v = PI[pos[m] * ROWS + a : pos[m] * ROWS + a + n, :]
        for c in cube.children(p, m):
            imsg(c, p).wait_recv()
            v = v + RI[pos[c] * ROWS + a : pos[c] * ROWS + a + n, :]
        PI[pos[m] * ROWS + a : pos[m] * ROWS + a + n, :] = v

    def oadd(m, p):
        a, n = tp[p]
        v = PT[0, pos[m], a : a + n, :]
        for c in cube.children(p, m):
            omsg(c, p).wait_recv()
            v = v + RT[pos[c], a : a + n, :]
        PT[0, pos[m], a : a + n, :] = v

    going = []

    def ready(m, msg):
        for p in cube.pieces:
            if m and not cube.children(p, m):
                c = msg(m, p)
                c.start()
                going.append(c)

    def follow(level, which):
        todo = [(m, p) for m in order if cube.level[m] == level for p in cube.pieces if cube.children(p, m)]
        for n in sorted({len(cube.children(p, m)) for m, p in todo}):
            for msg, add in [{"o": (omsg, oadd), "i": (imsg, iadd)}[w] for w in which]:
                for m, p in todo:
                    if len(cube.children(p, m)) == n:
                        add(m, p)
                        c = msg(m, p)
                        c.start()
                        going.append(c)

    pmsg = {
        m: send(PT.at[1, pos[m]], RTC.at[pos[m]], pcs.at[m], pcr.at[m], peer(0, "B", True)) for m in order
    }

    def pair(m):
        pmsg[m].wait_recv()
        PT[0, pos[m]] = PT[0, pos[m]] + RTC[pos[m]]
        ready(m, omsg)

    def weigh(r0, r1, c0, c1):
        for c in range(c0, c1):
            cols = slice(c * 256, (c + 1) * 256)
            cl = CROW[:, cols]
            for r in range(r0, r1, 64):
                at = slice(r, r + 64)
                v = L[at, cols]
                rl = RREP[at, :]
                w = jnp.exp2(v - jnp.concatenate([rl, rl], axis=1)) + jnp.exp2(v - cl)
                if c == 0 and r < 128:
                    across = lax.broadcasted_iota(jnp.int32, (64, 256), 1)
                    mark = lax.broadcasted_iota(jnp.int32, (64, 256), 0) + r == across
                    w = w - mark.astype(jnp.float32)
                W[at, cols] = w.astype(jnp.bfloat16)

    def text_grad(m):
        cols = slice(pos[m] * 256, (pos[m] + 1) * 256)
        v = jnp.dot(XT[...], W[:, cols], preferred_element_type=jnp.float32)
        PT[1, pos[m]] = v[:, 128:]
        PT[0, pos[m]] = v[:, :128]
        pmsg[m].start()

    def image_grad(first, last):
        at = slice(first * ROWS, last * ROWS)
        PI[at, :] = jnp.dot(W[at, :], T[...], preferred_element_type=jnp.float32)

    far = [(m, f) for m in range(nb) for f in (False, True) if m or f]
    stages = [
        [send(ST.at[0], ST.at[m], sts.at[m], str_.at[m], peer(m, "A")) for m in range(1, nb)],
        [send(ST.at[nb], ST.at[nb + 1 + i], sts.at[nb + i], str_.at[nb + i], peer(m, "B", f)) for i, (m, f) in enumerate(far)],
    ]

    def stat(at, copies):
        tile = ST[at]
        for j, c in enumerate(copies):
            c.wait_recv()
            tile = tile + ST[at + 1 + j]
        return tile

    def spread_scalars():
        part = -paired
        for r in range(0, rows, 128):
            at = slice(r, r + 128)
            part = part + jnp.sum((UR[at, :] * jnp.exp2(RM[at, :] - RREP[at, :])).reshape(16, 8, 128), axis=0)
        both = UC[...] * jnp.exp2(CM[...] - CROW[...])
        for c in range(0, 2 * rows, 128):
            part = part + both[:, c : c + 128]
        ST[0, :8] = loss_part
        ST[0, 8:] = part
        for c in stages[0]:
            c.start()

    spans = [(pos[ms[0]], pos[ms[-1]] + 1) for ms in levels]
    with jax.named_scope("farthest"):
        m = levels[nd][0]
        weigh(0, rows, pos[m], nb)
        text_grad(m)
        spread_scalars()
        weigh(pos[m] * ROWS, rows, 0, pos[m])
        image_grad(pos[m], nb)
        ready(m, imsg)
        waiting = [m]
    for lev in range(nd - 1, 1, -1):
        with jax.named_scope(f"middle{lev}"):
            first, last = spans[lev]
            weigh(0, last * ROWS, first, last)
            for m in levels[lev]:
                text_grad(m)
                if len(waiting) > 1 or waiting[0] == levels[nd][0]:
                    pair(waiting.pop(0))
                at = pos[m]
                weigh(at * ROWS, (at + 1) * ROWS, 0, first)
                image_grad(at, at + 1)
                ready(m, imsg)
                waiting.append(m)
            while waiting:
                pair(waiting.pop(0))
    with jax.named_scope("near"):
        first, last = spans[1] if nd > 1 else (1, 1)
        weigh(0, last * ROWS, 0, last)
        for m in levels[1] if nd > 1 else []:
            text_grad(m)
    with jax.named_scope("stats"):
        ST[nb] = stat(0, stages[0])
        for c in stages[1]:
            c.start()
    with jax.named_scope("nearimages"):
        while waiting:
            pair(waiting.pop(0))
        if nd > 1:
            image_grad(first, last)
            follow(nd - 1, "i")
            for m in levels[1]:
                ready(m, imsg)
            follow(nd - 1, "o")
        for m in levels[1] if nd > 1 else []:
            pair(m)
    with jax.named_scope("own"):
        text_grad(0)
        image_grad(0, 1)
        pair(0)
    with jax.named_scope("follow"):
        for lev in range(nd - 2, 0, -1):
            follow(lev, "oi")
    with jax.named_scope("last"):
        for p in cube.pieces:
            oadd(0, p)
        gt_out[...] = (PT[0, 0] * scale).T.astype(jnp.bfloat16)
        for p in cube.pieces:
            iadd(0, p)
        gi_out[...] = (PI[:128, :] * scale[:, :1]).astype(jnp.bfloat16)
        tile = stat(nb, stages[1])
        loss = jnp.sum(tile[:8]) * (LN2 * 0.5 / total)
        grad_scale = jnp.sum(tile[8:]) * (LN2 / total)
        stats_out[...] = jnp.where(line == 0, loss, grad_scale)
        for c in going + list(pmsg.values()) + stages[0] + stages[1]:
            c.wait_send()


def hand_over(gi, gt, stats, gi_out, gt_out, loss_out, scale_out):
    gi_out[...] = gi[...]
    gt_out[...] = gt[...]
    loss_out[...] = stats[0:1, 0:1]
    scale_out[...] = stats[1:2, 0:1]


def body(dims, total, images, texts, log_scale):
    nd = len(dims)
    nb = 2**nd
    f32, bf16 = jnp.float32, jnp.bfloat16
    vm, dma = pltpu.VMEM, pltpu.SemaphoreType.DMA
    width = images.shape[1]
    rows, cols = nb * ROWS, 2 * nb * ROWS
    gi, gt, stats = pl.pallas_call(
        functools.partial(kernel, dims, total),
        out_shape=(
            jax.ShapeDtypeStruct(images.shape, bf16),
            jax.ShapeDtypeStruct(texts.shape, bf16),
            jax.ShapeDtypeStruct((8, 128), f32),
        ),
        in_specs=[
            pl.BlockSpec(memory_space=pltpu.SMEM),
            pl.BlockSpec(memory_space=pl.ANY),
            pl.BlockSpec(memory_space=pl.ANY),
        ],
        out_specs=(pl.BlockSpec(memory_space=vm),) * 3,
        scratch_shapes=[
            vm((rows, width), bf16), vm((width, rows), bf16), vm((cols, width), bf16),
            vm((rows, cols), f32), vm((rows, cols), bf16),
            vm((rows, 128), f32), vm((rows, 128), f32), vm((rows, 128), f32), vm((rows, 128), f32),
            vm((8, cols), f32), vm((8, cols), f32), vm((8, cols), f32), vm((8, cols), f32),
            vm((nb, nb, 128), f32), vm((2 * nb, 2 * nb, 128), f32), vm((rows, 128), f32), vm((1, cols), f32),
            vm((rows, width), f32), vm((rows, width), f32),
            vm((2, nb, width, 128), f32), vm((nb, width, 128), f32), vm((nb, width, 128), f32),
            vm((3 * nb, 16, 128), f32),
            dma((2,)), dma((nb, nd)), dma((nb, nd)), dma((nb, nd)), dma((nb, nd)), dma((nb, nd)), dma((nb, nd)),
            dma((nb,)), dma((nb,)), dma((2 * nb,)), dma((2 * nb,)),
            dma((nb, nd)), dma((nb, nd)), dma((nb,)), dma((nb,)), dma((nb, nd)), dma((nb, nd)),
            dma((3 * nb,)), dma((3 * nb,)),
        ],
        compiler_params=pltpu.CompilerParams(
            collective_id=0, has_side_effects=True, vmem_limit_bytes=60 * 2**20
        ),
        name="contrastive",
    )(log_scale, images, texts)
    outs = pl.pallas_call(
        hand_over,
        out_shape=(
            jax.ShapeDtypeStruct(images.shape, bf16),
            jax.ShapeDtypeStruct(texts.shape, bf16),
            jax.ShapeDtypeStruct((1, 1), f32),
            jax.ShapeDtypeStruct((1, 1), f32),
        ),
        in_specs=[pl.BlockSpec(memory_space=vm)] * 3,
        out_specs=(pl.BlockSpec(memory_space=vm),) * 4,
        name="outputs",
    )(gi, gt, stats)
    return outs[0], outs[1], outs[2].reshape(()), outs[3].reshape(())


def solution(mesh):
    return build(Mesh(mesh.devices.reshape(4, 4, 2, 4), AXES))


def build(split):
    dims = tuple(a for a in CUBE if split.shape[a] == 4)
    placed = P(AXES, None)
    return jax.shard_map(
        functools.partial(body, dims, ROWS * split.size),
        mesh=split,
        in_specs=(placed, placed, P()),
        out_specs=(placed, placed, P(), P()),
        check_vma=False,
    )
```

```python
import functools
import math

import jax
import jax.numpy as jnp
from jax import lax
from jax.experimental import pallas as pl
from jax.experimental.pallas import tpu as pltpu
from jax.sharding import Mesh
from jax.sharding import PartitionSpec as P

AXES = ("x", "y", "core", "z")
CUBE = ("x", "y", "z")
MESH = pl.DeviceIdType.MESH
ROWS = 128
LOG2E = math.log2(math.e)
LN2 = math.log(2.0)
NT = (((1,), (1,)), ((), ()))


class Cube:
    def __init__(self, n):
        self.n = n
        self.order = sorted(range(2**n), key=lambda m: (bin(m).count("1"), m))
        self.pos = {m: i for i, m in enumerate(self.order)}
        self.level = {m: bin(m).count("1") for m in self.order}
        self.pieces = range(n)

    def hop(self, p, m):
        return next(k % self.n for k in range(p, p + self.n) if m >> (k % self.n) & 1)

    def children(self, p, m):
        more = [(k, m | 1 << k) for k in range(self.n) if not m >> k & 1]
        return [c for k, c in more if self.hop(p, c) == k]

    def turns(self):
        seen = []
        for q in (1, -1, 0):
            if q % self.n not in seen:
                seen.append(q % self.n)
        return seen


def cut(total, n, unit):
    units = total // unit
    ends = [-(-units * i // n) * unit for i in range(n + 1)]
    return [(a, b - a) for a, b in zip(ends, ends[1:])]


def kernel(
    dims, total,
    log_scale, images, texts,
    gi_out, gt_out, stats_out,
    X, XT, T, L, W, RM, RN, RS, UR, CM, CN, CS, UC, RL, CL, RREP, CROW,
    PI, RI, PT, RTC, RT, ST,
    local_sem, xs, xr, ts, tr, ds, dr, rls, rlr, cls, clr, pis, pir, pcs, pcr, pts, ptr, sts, str_,
):
    nd = len(dims)
    nb = 2**nd
    rows = nb * ROWS
    cube = Cube(nd)
    order, pos = cube.order, cube.pos
    me = {a: lax.axis_index(a) for a in AXES}
    core = me["core"]

    def peer(mask, kind, flip=False):
        ident = {}
        for d, a in enumerate(dims):
            if mask >> d & 1:
                c = me[a]
                ident[a] = 3 - c if kind == "A" else c + 1 - 2 * (c % 2)
        if flip:
            ident["core"] = 1 - core
        return ident

    def spot(mask, kind):
        at = 0
        for d, a in enumerate(dims):
            bit = me[a] // 2 if kind == "A" else me[a] % 2
            at = at + 2**d * (1 - bit if mask >> d & 1 else bit)
        return at

    def send(src, dst, s, r, where):
        return pltpu.make_async_remote_copy(
            src_ref=src, dst_ref=dst, send_sem=s, recv_sem=r, device_id=where, device_id_type=MESH
        )

    with jax.named_scope("enter"):
        ci = pltpu.make_async_copy(images, X.at[pl.ds(0, ROWS)], local_sem.at[0])
        ct = pltpu.make_async_copy(texts, T.at[pl.ds(0, ROWS)], local_sem.at[1])
        ci.start()
        ct.start()
        barrier = pltpu.get_barrier_semaphore()
        others = [(1 << k, kind, False) for k in range(nd) for kind in "AB"] + [(0, "B", True)]
        for o in others:
            pl.semaphore_signal(barrier, inc=1, device_id=peer(*o), device_id_type=MESH)
        RM[...] = jnp.full(RM.shape, -3e38, jnp.float32)
        RS[...] = jnp.zeros(RS.shape, jnp.float32)
        CM[...] = jnp.full(CM.shape, -3e38, jnp.float32)
        CS[...] = jnp.zeros(CS.shape, jnp.float32)
        UR[...] = jnp.zeros(UR.shape, jnp.float32)
        scale = jnp.exp(jnp.full((1, 128), log_scale[()], jnp.float32))
        scale_two = jnp.concatenate([scale * LOG2E] * 2, axis=1)
        ci.wait()
        ct.wait()
        pl.semaphore_wait(barrier, len(others))

    gp = cut(ROWS, nd, 16)
    started = []

    def go(c):
        c.start()
        started.append(c)

    def xmsg(m, p):
        k = cube.hop(p, m)
        a, n = gp[p]
        src = X.at[pl.ds(pos[m ^ 1 << k] * ROWS + a, n)]
        return send(src, X.at[pl.ds(pos[m] * ROWS + a, n)], xs.at[m, p], xr.at[m, p], peer(1 << k, "A"))

    def tmsg(m, p):
        k = cube.hop(p, m)
        a, n = gp[p]
        src = T.at[pl.ds(pos[m ^ 1 << k] * 2 * ROWS + a, n)]
        return send(src, T.at[pl.ds(pos[m] * 2 * ROWS + a, n)], ts.at[m, p], tr.at[m, p], peer(1 << k, "B"))

    def dmsg(m, p):
        a, n = gp[p]
        at = pos[m] * 2 * ROWS + a
        return send(T.at[pl.ds(at, n)], T.at[pl.ds(at + ROWS, n)], ds.at[m, p], dr.at[m, p], peer(0, "B", True))

    def pass_on(events):
        nxt = [(c, p) for m, p in events for c in cube.children(p, m)]
        nxt.sort(key=lambda e: not cube.children(e[1], e[0]))
        for m, p in events:
            tmsg(m, p).wait_recv()
        for e in nxt:
            go(tmsg(*e))
        for e in events:
            go(dmsg(*e))
        for m, p in events:
            xmsg(m, p).wait_recv()
        for e in nxt:
            go(xmsg(*e))

    def logits(r0, r1, c0, c1):
        for i in range(c0, c1):
            cols = slice(i * 256, (i + 1) * 256)
            v = lax.dot_general(X[r0:r1, :], T[cols, :], NT, preferred_element_type=jnp.float32) * scale_two
            L[r0:r1, cols] = v
            RN[r0:r1, :] = jnp.maximum(RN[r0:r1, :], jnp.maximum(v[:, :128], v[:, 128:]))
            CN[:, cols] = jnp.maximum(CN[:, cols], jnp.max(v.reshape(-1, 8, 256), axis=0))

    def new_tops(r0, r1, c0, c1):
        at = slice(r0, r1)
        RS[at, :] = RS[at, :] * jnp.exp2(RM[at, :] - RN[at, :])
        RM[at, :] = RN[at, :]
        cols = slice(c0 * 256, c1 * 256)
        CS[:, cols] = CS[:, cols] * jnp.exp2(CM[:, cols] - CN[:, cols])
        CM[:, cols] = CN[:, cols]

    def sums(r0, r1, c0, c1):
        def step(i, _):
            cols = pl.ds(pl.multiple_of(i * 256, 256), 256)
            cm = CM[:, cols]
            cs = CS[:, cols]
            for r in range(r0, r1, 64):
                at = slice(r, r + 64)
                v = L[at, cols]
                rm = RM[at, :]
                er0 = jnp.exp2(v[:, :128] - rm)
                er1 = jnp.exp2(v[:, 128:] - rm)
                RS[at, :] = RS[at, :] + (er0 + er1)
                ec = jnp.exp2(v.reshape(8, 8, 256) - cm)
                cs = cs + jnp.sum(ec, axis=0)
            CS[:, cols] = cs
            return 0

        lax.fori_loop(c0, c1, step, 0)

    def partner_texts(masks):
        for m in masks:
            for p in cube.pieces:
                dmsg(m, p).wait_recv()

    with jax.named_scope("gather"):
        for p in cube.pieces:
            go(dmsg(0, p))
        for q in cube.turns():
            for k in range(nd):
                go(xmsg(1 << k, (k + q) % nd))
                go(tmsg(1 << k, (k + q) % nd))
        levels = [[m for m in order if cube.level[m] == i] for i in range(nd + 1)]
        RN[...] = RM[...]
        CN[...] = CM[...]
        partner_texts(levels[0])
        logits(0, ROWS, 0, 1)
        new_tops(0, ROWS, 0, 1)
        sums(0, ROWS, 0, 1)
        groups = [[(1 << k, (k + q) % nd) for k in range(nd)] for q in cube.turns()]
        for g in groups:
            pass_on(g)
    for lev in range(1, nd + 1):
        before = sum(len(levels[i]) for i in range(lev))
        done = before + len(levels[lev])
        old, new = before * ROWS, done * ROWS
        with jax.named_scope(f"gather{lev}"):
            if 1 < lev < nd:
                events = [(m, p) for m in levels[lev] for p in cube.pieces]
                deep = [e for e in events if cube.children(e[1], e[0])]
                if deep:
                    pass_on(deep)
                pass_on([e for e in events if e not in deep])
            elif lev > 1:
                pass_on([(m, p) for m in levels[lev] for p in cube.pieces])
        with jax.named_scope(f"rows{lev}"):
            logits(old, new, 0, before)
            new_tops(old, new, 0, before)
            sums(old, new, 0, before)
        with jax.named_scope(f"partner{lev}"):
            partner_texts(levels[lev])
        with jax.named_scope(f"columns{lev}"):
            logits(0, new, before, done)
            new_tops(0, new, before, done)
            sums(0, new, before, done)

    with jax.named_scope("lse"):
        ctop = jnp.max(CM[...], axis=0, keepdims=True)
        ccol = ctop + jnp.log2(jnp.sum(CS[...] * jnp.exp2(CM[...] - ctop), axis=0, keepdims=True))
        for m in order:
            for f in range(2):
                at = (2 * pos[m] + f) * 128
                line = (1 - core if f else core) * nb + spot(m, "B")
                CL[0, pl.ds(line, 1), :] = ccol[:, at : at + 128]
        cc = [
            send(CL.at[0], CL.at[2 * m + f], cls.at[2 * m + f], clr.at[2 * m + f], peer(m, "B", f == 1))
            for m in reversed(order) for f in range(2) if m or f
        ]
        for c in cc:
            c.start()
        for m in order:
            at = slice(pos[m] * 128, (pos[m] + 1) * 128)
            tops = RM[at, :].T
            top = jnp.max(tops, axis=0, keepdims=True)
            part = jnp.sum(RS[at, :].T * jnp.exp2(tops - top), axis=0, keepdims=True)
            RL[0, pl.ds(spot(m, "A"), 1), :] = top + jnp.log2(part)
        rc = [send(RL.at[0], RL.at[m], rls.at[m], rlr.at[m], peer(m, "A")) for m in reversed(order[1:])]
        for c in rc:
            c.start()
    with jax.named_scope("turn"):
        def tilt(c, _):
            cols = pl.ds(pl.multiple_of(c * 256, 256), 256)
            cm = CM[:, cols]

            def strip(i, uc):
                at = pl.ds(pl.multiple_of(i * 256, 256), 256)
                v = L[at, cols]
                rm = RM[at, :]
                v0, v1 = v[:, :128], v[:, 128:]
                UR[at, :] = UR[at, :] + (jnp.exp2(v0 - rm) * v0 + jnp.exp2(v1 - rm) * v1)
                w = v.reshape(32, 8, 256)
                return uc + jnp.sum(jnp.exp2(w - cm) * w, axis=0)

            UC[:, cols] = lax.fori_loop(0, rows // 256, strip, jnp.zeros((8, 256), jnp.float32))
            return 0

        lax.fori_loop(0, nb, tilt, 0)
        XT[...] = X[...].T
        for c in started:
            c.wait_send()
    with jax.named_scope("lsewait"):
        for c in cc + rc:
            c.wait_recv()
        for c in cc + rc:
            c.wait_send()

    with jax.named_scope("join"):
        def joined(parts):
            top = functools.reduce(jnp.maximum, parts)
            return top + jnp.log2(functools.reduce(jnp.add, [jnp.exp2(p - top) for p in parts]))

        RL[0] = joined([RL[m] for m in range(nb)])
        CL[0] = joined([CL[m] for m in range(2 * nb)])
        for m in order:
            line = RL[0, pl.ds(spot(m, "A"), 1), :]
            RREP[pos[m] * 128 : (pos[m] + 1) * 128, :] = jnp.broadcast_to(line + 1.0, (128, 128)).T
            for f in range(2):
                at = (2 * pos[m] + f) * 128
                CROW[:, at : at + 128] = CL[0, pl.ds((1 - core if f else core) * nb + spot(m, "B"), 1), :] + 1.0
        eye = lax.broadcasted_iota(jnp.int32, (128, 128), 0) == lax.broadcasted_iota(jnp.int32, (128, 128), 1)
        paired = jnp.sum(jnp.where(eye, L[:128, :128], 0.0).reshape(16, 8, 128), axis=0)
        line = lax.broadcasted_iota(jnp.int32, (8, 128), 0)
        own = RL[0, pl.ds(spot(0, "A"), 1), :] + CL[0, pl.ds(core * nb + spot(0, "B"), 1), :]
        loss_part = jnp.where(line == 0, own, 0.0) - 2.0 * paired

    ip = cut(ROWS, nd, 8)
    tp = cut(XT.shape[0], nd, 8)

    def imsg(m, p):
        k = cube.hop(p, m)
        a, n = ip[p]
        at = pl.ds(pos[m] * ROWS + a, n)
        return send(PI.at[at], RI.at[at], pis.at[m, p], pir.at[m, p], peer(1 << k, "A"))

    def omsg(m, p):
        k = cube.hop(p, m)
        a, n = tp[p]
        at = pl.ds(a, n)
        return send(PT.at[0, pos[m], at], RT.at[pos[m], at], pts.at[m, p], ptr.at[m, p], peer(1 << k, "B"))

    def iadd(m, p):
        a, n = ip[p]
        v = PI[pos[m] * ROWS + a : pos[m] * ROWS + a + n, :]
        for c in cube.children(p, m):
            imsg(c, p).wait_recv()
            v = v + RI[pos[c] * ROWS + a : pos[c] * ROWS + a + n, :]
        PI[pos[m] * ROWS + a : pos[m] * ROWS + a + n, :] = v

    def oadd(m, p):
        a, n = tp[p]
        v = PT[0, pos[m], a : a + n, :]
        for c in cube.children(p, m):
            omsg(c, p).wait_recv()
            v = v + RT[pos[c], a : a + n, :]
        PT[0, pos[m], a : a + n, :] = v

    going = []

    def ready(m, msg):
        for p in cube.pieces:
            if m and not cube.children(p, m):
                c = msg(m, p)
                c.start()
                going.append(c)

    def follow(level, which):
        todo = [(m, p) for m in order if cube.level[m] == level for p in cube.pieces if cube.children(p, m)]
        for n in sorted({len(cube.children(p, m)) for m, p in todo}):
            for msg, add in [{"o": (omsg, oadd), "i": (imsg, iadd)}[w] for w in which]:
                for m, p in todo:
                    if len(cube.children(p, m)) == n:
                        add(m, p)
                        c = msg(m, p)
                        c.start()
                        going.append(c)

    pmsg = {
        m: send(PT.at[1, pos[m]], RTC.at[pos[m]], pcs.at[m], pcr.at[m], peer(0, "B", True)) for m in order
    }

    def pair(m):
        pmsg[m].wait_recv()
        PT[0, pos[m]] = PT[0, pos[m]] + RTC[pos[m]]
        ready(m, omsg)

    def weigh(r0, r1, c0, c1):
        for c in range(c0, c1):
            cols = slice(c * 256, (c + 1) * 256)
            cl = CROW[:, cols]
            for r in range(r0, r1, 64):
                at = slice(r, r + 64)
                v = L[at, cols]
                rl = RREP[at, :]
                w = jnp.exp2(v - jnp.concatenate([rl, rl], axis=1)) + jnp.exp2(v - cl)
                if c == 0 and r < 128:
                    across = lax.broadcasted_iota(jnp.int32, (64, 256), 1)
                    mark = lax.broadcasted_iota(jnp.int32, (64, 256), 0) + r == across
                    w = w - mark.astype(jnp.float32)
                W[at, cols] = w.astype(jnp.bfloat16)

    def text_grad(m):
        cols = slice(pos[m] * 256, (pos[m] + 1) * 256)
        v = jnp.dot(XT[...], W[:, cols], preferred_element_type=jnp.float32)
        PT[1, pos[m]] = v[:, 128:]
        PT[0, pos[m]] = v[:, :128]
        pmsg[m].start()

    def image_grad(first, last):
        at = slice(first * ROWS, last * ROWS)
        PI[at, :] = jnp.dot(W[at, :], T[...], preferred_element_type=jnp.float32)

    far = [(m, f) for m in range(nb) for f in (False, True) if m or f]
    stages = [
        [send(ST.at[0], ST.at[m], sts.at[m], str_.at[m], peer(m, "A")) for m in range(1, nb)],
        [send(ST.at[nb], ST.at[nb + 1 + i], sts.at[nb + i], str_.at[nb + i], peer(m, "B", f)) for i, (m, f) in enumerate(far)],
    ]

    def stat(at, copies):
        tile = ST[at]
        for j, c in enumerate(copies):
            c.wait_recv()
            tile = tile + ST[at + 1 + j]
        return tile

    def spread_scalars():
        part = -paired
        for r in range(0, rows, 128):
            at = slice(r, r + 128)
            part = part + jnp.sum((UR[at, :] * jnp.exp2(RM[at, :] - RREP[at, :])).reshape(16, 8, 128), axis=0)
        both = UC[...] * jnp.exp2(CM[...] - CROW[...])
        for c in range(0, 2 * rows, 128):
            part = part + both[:, c : c + 128]
        ST[0, :8] = loss_part
        ST[0, 8:] = part
        for c in stages[0]:
            c.start()

    spans = [(pos[ms[0]], pos[ms[-1]] + 1) for ms in levels]
    with jax.named_scope("farthest"):
        m = levels[nd][0]
        weigh(0, rows, pos[m], nb)
        text_grad(m)
        spread_scalars()
        weigh(pos[m] * ROWS, rows, 0, pos[m])
        image_grad(pos[m], nb)
        ready(m, imsg)
        waiting = [m]
    for lev in range(nd - 1, 1, -1):
        with jax.named_scope(f"middle{lev}"):
            first, last = spans[lev]
            weigh(0, last * ROWS, first, last)
            for m in levels[lev]:
                text_grad(m)
                if len(waiting) > 1 or waiting[0] == levels[nd][0]:
                    pair(waiting.pop(0))
                at = pos[m]
                weigh(at * ROWS, (at + 1) * ROWS, 0, first)
                image_grad(at, at + 1)
                ready(m, imsg)
                waiting.append(m)
            while waiting:
                pair(waiting.pop(0))
    with jax.named_scope("near"):
        first, last = spans[1] if nd > 1 else (1, 1)
        weigh(0, last * ROWS, 0, last)
        for m in levels[1] if nd > 1 else []:
            text_grad(m)
    with jax.named_scope("stats"):
        ST[nb] = stat(0, stages[0])
        for c in stages[1]:
            c.start()
    with jax.named_scope("nearimages"):
        while waiting:
            pair(waiting.pop(0))
        if nd > 1:
            image_grad(first, last)
            follow(nd - 1, "i")
            for m in levels[1]:
                ready(m, imsg)
            follow(nd - 1, "o")
        for m in levels[1] if nd > 1 else []:
            pair(m)
    with jax.named_scope("own"):
        text_grad(0)
        image_grad(0, 1)
        pair(0)
    with jax.named_scope("follow"):
        for lev in range(nd - 2, 0, -1):
            follow(lev, "oi")
    with jax.named_scope("last"):
        for p in cube.pieces:
            iadd(0, p)
        gi_out[...] = (PI[:128, :] * scale[:, :1]).astype(jnp.bfloat16)
        tile = stat(nb, stages[1])
        loss = jnp.sum(tile[:8]) * (LN2 * 0.5 / total)
        grad_scale = jnp.sum(tile[8:]) * (LN2 / total)
        stats_out[...] = jnp.where(line == 0, loss, grad_scale)
    with jax.named_scope("lasttexts"):
        for p in cube.pieces:
            oadd(0, p)
        gt_out[...] = (PT[0, 0] * scale).T.astype(jnp.bfloat16)
        for c in going + list(pmsg.values()) + stages[0] + stages[1]:
            c.wait_send()


def hand_over(gi, gt, stats, gi_out, gt_out, loss_out, scale_out):
    gi_out[...] = gi[...]
    gt_out[...] = gt[...]
    loss_out[...] = stats[0:1, 0:1]
    scale_out[...] = stats[1:2, 0:1]


def body(dims, total, images, texts, log_scale):
    nd = len(dims)
    nb = 2**nd
    f32, bf16 = jnp.float32, jnp.bfloat16
    vm, dma = pltpu.VMEM, pltpu.SemaphoreType.DMA
    width = images.shape[1]
    rows, cols = nb * ROWS, 2 * nb * ROWS
    gi, gt, stats = pl.pallas_call(
        functools.partial(kernel, dims, total),
        out_shape=(
            jax.ShapeDtypeStruct(images.shape, bf16),
            jax.ShapeDtypeStruct(texts.shape, bf16),
            jax.ShapeDtypeStruct((8, 128), f32),
        ),
        in_specs=[
            pl.BlockSpec(memory_space=pltpu.SMEM),
            pl.BlockSpec(memory_space=pl.ANY),
            pl.BlockSpec(memory_space=pl.ANY),
        ],
        out_specs=(pl.BlockSpec(memory_space=vm),) * 3,
        scratch_shapes=[
            vm((rows, width), bf16), vm((width, rows), bf16), vm((cols, width), bf16),
            vm((rows, cols), f32), vm((rows, cols), bf16),
            vm((rows, 128), f32), vm((rows, 128), f32), vm((rows, 128), f32), vm((rows, 128), f32),
            vm((8, cols), f32), vm((8, cols), f32), vm((8, cols), f32), vm((8, cols), f32),
            vm((nb, nb, 128), f32), vm((2 * nb, 2 * nb, 128), f32), vm((rows, 128), f32), vm((1, cols), f32),
            vm((rows, width), f32), vm((rows, width), f32),
            vm((2, nb, width, 128), f32), vm((nb, width, 128), f32), vm((nb, width, 128), f32),
            vm((3 * nb, 16, 128), f32),
            dma((2,)), dma((nb, nd)), dma((nb, nd)), dma((nb, nd)), dma((nb, nd)), dma((nb, nd)), dma((nb, nd)),
            dma((nb,)), dma((nb,)), dma((2 * nb,)), dma((2 * nb,)),
            dma((nb, nd)), dma((nb, nd)), dma((nb,)), dma((nb,)), dma((nb, nd)), dma((nb, nd)),
            dma((3 * nb,)), dma((3 * nb,)),
        ],
        compiler_params=pltpu.CompilerParams(
            collective_id=0, has_side_effects=True, vmem_limit_bytes=60 * 2**20
        ),
        name="contrastive",
    )(log_scale, images, texts)
    outs = pl.pallas_call(
        hand_over,
        out_shape=(
            jax.ShapeDtypeStruct(images.shape, bf16),
            jax.ShapeDtypeStruct(texts.shape, bf16),
            jax.ShapeDtypeStruct((1, 1), f32),
            jax.ShapeDtypeStruct((1, 1), f32),
        ),
        in_specs=[pl.BlockSpec(memory_space=vm)] * 3,
        out_specs=(pl.BlockSpec(memory_space=vm),) * 4,
        name="outputs",
    )(gi, gt, stats)
    return outs[0], outs[1], outs[2].reshape(()), outs[3].reshape(())


def solution(mesh):
    return build(Mesh(mesh.devices.reshape(4, 4, 2, 4), AXES))


def build(split):
    dims = tuple(a for a in CUBE if split.shape[a] == 4)
    placed = P(AXES, None)
    return jax.shard_map(
        functools.partial(body, dims, ROWS * split.size),
        mesh=split,
        in_specs=(placed, placed, P()),
        out_specs=(placed, placed, P(), P()),
        check_vma=False,
    )
```

```python
import functools
import math

import jax
import jax.numpy as jnp
from jax import lax
from jax.experimental import pallas as pl
from jax.experimental.pallas import tpu as pltpu
from jax.sharding import Mesh
from jax.sharding import PartitionSpec as P

AXES = ("x", "y", "core", "z")
CUBE = ("x", "y", "z")
MESH = pl.DeviceIdType.MESH
ROWS = 128
LOG2E = math.log2(math.e)
LN2 = math.log(2.0)
NT = (((1,), (1,)), ((), ()))


class Cube:
    def __init__(self, n):
        self.n = n
        self.order = sorted(range(2**n), key=lambda m: (bin(m).count("1"), m))
        self.pos = {m: i for i, m in enumerate(self.order)}
        self.level = {m: bin(m).count("1") for m in self.order}
        self.pieces = range(n)

    def hop(self, p, m):
        return next(k % self.n for k in range(p, p + self.n) if m >> (k % self.n) & 1)

    def children(self, p, m):
        more = [(k, m | 1 << k) for k in range(self.n) if not m >> k & 1]
        return [c for k, c in more if self.hop(p, c) == k]

    def turns(self):
        seen = []
        for q in (1, -1, 0):
            if q % self.n not in seen:
                seen.append(q % self.n)
        return seen


def cut(total, n, unit):
    units = total // unit
    ends = [-(-units * i // n) * unit for i in range(n + 1)]
    return [(a, b - a) for a, b in zip(ends, ends[1:])]


def kernel(
    dims, total,
    log_scale, images, texts,
    gi_out, gt_out, stats_out,
    X, XT, T, L, W, RM, RN, RS, UR, CM, CN, CS, UC, RL, CL, RREP, CROW,
    PI, RI, PT, RTC, RT, ST,
    local_sem, xs, xr, ts, tr, ds, dr, rls, rlr, cls, clr, pis, pir, pcs, pcr, pts, ptr, sts, str_,
):
    nd = len(dims)
    nb = 2**nd
    rows = nb * ROWS
    cube = Cube(nd)
    order, pos = cube.order, cube.pos
    me = {a: lax.axis_index(a) for a in AXES}
    core = me["core"]

    def peer(mask, kind, flip=False):
        ident = {}
        for d, a in enumerate(dims):
            if mask >> d & 1:
                c = me[a]
                ident[a] = 3 - c if kind == "A" else c + 1 - 2 * (c % 2)
        if flip:
            ident["core"] = 1 - core
        return ident

    def spot(mask, kind):
        at = 0
        for d, a in enumerate(dims):
            bit = me[a] // 2 if kind == "A" else me[a] % 2
            at = at + 2**d * (1 - bit if mask >> d & 1 else bit)
        return at

    def send(src, dst, s, r, where):
        return pltpu.make_async_remote_copy(
            src_ref=src, dst_ref=dst, send_sem=s, recv_sem=r, device_id=where, device_id_type=MESH
        )

    with jax.named_scope("enter"):
        ci = pltpu.make_async_copy(images, X.at[pl.ds(0, ROWS)], local_sem.at[0])
        ct = pltpu.make_async_copy(texts, T.at[pl.ds(0, ROWS)], local_sem.at[1])
        ci.start()
        ct.start()
        barrier = pltpu.get_barrier_semaphore()
        others = [(1 << k, kind, False) for k in range(nd) for kind in "AB"] + [(0, "B", True)]
        for o in others:
            pl.semaphore_signal(barrier, inc=1, device_id=peer(*o), device_id_type=MESH)
        RM[...] = jnp.full(RM.shape, -3e38, jnp.float32)
        RS[...] = jnp.zeros(RS.shape, jnp.float32)
        CM[...] = jnp.full(CM.shape, -3e38, jnp.float32)
        CS[...] = jnp.zeros(CS.shape, jnp.float32)
        UR[...] = jnp.zeros(UR.shape, jnp.float32)
        scale = jnp.exp(jnp.full((1, 128), log_scale[()], jnp.float32))
        scale_two = jnp.concatenate([scale * LOG2E] * 2, axis=1)
        ci.wait()
        ct.wait()
        pl.semaphore_wait(barrier, len(others))

    gp = cut(ROWS, nd, 16)
    started = []

    def go(c):
        c.start()
        started.append(c)

    def xmsg(m, p):
        k = cube.hop(p, m)
        a, n = gp[p]
        src = X.at[pl.ds(pos[m ^ 1 << k] * ROWS + a, n)]
        return send(src, X.at[pl.ds(pos[m] * ROWS + a, n)], xs.at[m, p], xr.at[m, p], peer(1 << k, "A"))

    def tmsg(m, p):
        k = cube.hop(p, m)
        a, n = gp[p]
        src = T.at[pl.ds(pos[m ^ 1 << k] * 2 * ROWS + a, n)]
        return send(src, T.at[pl.ds(pos[m] * 2 * ROWS + a, n)], ts.at[m, p], tr.at[m, p], peer(1 << k, "B"))

    def dmsg(m, p):
        a, n = gp[p]
        at = pos[m] * 2 * ROWS + a
        return send(T.at[pl.ds(at, n)], T.at[pl.ds(at + ROWS, n)], ds.at[m, p], dr.at[m, p], peer(0, "B", True))

    def pass_on(events):
        nxt = [(c, p) for m, p in events for c in cube.children(p, m)]
        nxt.sort(key=lambda e: not cube.children(e[1], e[0]))
        for m, p in events:
            tmsg(m, p).wait_recv()
        for e in nxt:
            go(tmsg(*e))
        for e in events:
            go(dmsg(*e))
        for m, p in events:
            xmsg(m, p).wait_recv()
        for e in nxt:
            go(xmsg(*e))

    def logits(r0, r1, c0, c1):
        for i in range(c0, c1):
            cols = slice(i * 256, (i + 1) * 256)
            v = lax.dot_general(X[r0:r1, :], T[cols, :], NT, preferred_element_type=jnp.float32) * scale_two
            L[r0:r1, cols] = v
            RN[r0:r1, :] = jnp.maximum(RN[r0:r1, :], jnp.maximum(v[:, :128], v[:, 128:]))
            CN[:, cols] = jnp.maximum(CN[:, cols], jnp.max(v.reshape(-1, 8, 256), axis=0))

    def new_tops(r0, r1, c0, c1):
        at = slice(r0, r1)
        RS[at, :] = RS[at, :] * jnp.exp2(RM[at, :] - RN[at, :])
        RM[at, :] = RN[at, :]
        cols = slice(c0 * 256, c1 * 256)
        CS[:, cols] = CS[:, cols] * jnp.exp2(CM[:, cols] - CN[:, cols])
        CM[:, cols] = CN[:, cols]

    def sums(r0, r1, c0, c1):
        def step(i, _):
            cols = pl.ds(pl.multiple_of(i * 256, 256), 256)
            cm = CM[:, cols]
            cs = CS[:, cols]
            for r in range(r0, r1, 64):
                at = slice(r, r + 64)
                v = L[at, cols]
                rm = RM[at, :]
                er0 = jnp.exp2(v[:, :128] - rm)
                er1 = jnp.exp2(v[:, 128:] - rm)
                RS[at, :] = RS[at, :] + (er0 + er1)
                ec = jnp.exp2(v.reshape(8, 8, 256) - cm)
                cs = cs + jnp.sum(ec, axis=0)
            CS[:, cols] = cs
            return 0

        lax.fori_loop(c0, c1, step, 0)

    def partner_texts(masks):
        for m in masks:
            for p in cube.pieces:
                dmsg(m, p).wait_recv()

    with jax.named_scope("gather"):
        for p in cube.pieces:
            go(dmsg(0, p))
        for q in cube.turns():
            for k in range(nd):
                go(xmsg(1 << k, (k + q) % nd))
                go(tmsg(1 << k, (k + q) % nd))
        levels = [[m for m in order if cube.level[m] == i] for i in range(nd + 1)]
        RN[...] = RM[...]
        CN[...] = CM[...]
        partner_texts(levels[0])
        logits(0, ROWS, 0, 1)
        new_tops(0, ROWS, 0, 1)
        sums(0, ROWS, 0, 1)
        groups = [[(1 << k, (k + q) % nd) for k in range(nd)] for q in cube.turns()]
        for g in groups:
            pass_on(g)
    for lev in range(1, nd + 1):
        before = sum(len(levels[i]) for i in range(lev))
        done = before + len(levels[lev])
        old, new = before * ROWS, done * ROWS
        with jax.named_scope(f"gather{lev}"):
            if 1 < lev < nd:
                events = [(m, p) for m in levels[lev] for p in cube.pieces]
                deep = [e for e in events if cube.children(e[1], e[0])]
                if deep:
                    pass_on(deep)
                pass_on([e for e in events if e not in deep])
            elif lev > 1:
                pass_on([(m, p) for m in levels[lev] for p in cube.pieces])
        with jax.named_scope(f"rows{lev}"):
            logits(old, new, 0, before)
            new_tops(old, new, 0, before)
            sums(old, new, 0, before)
        with jax.named_scope(f"partner{lev}"):
            partner_texts(levels[lev])
        with jax.named_scope(f"columns{lev}"):
            logits(0, new, before, done)
            new_tops(0, new, before, done)
            sums(0, new, before, done)

    with jax.named_scope("lse"):
        ctop = jnp.max(CM[...], axis=0, keepdims=True)
        ccol = ctop + jnp.log2(jnp.sum(CS[...] * jnp.exp2(CM[...] - ctop), axis=0, keepdims=True))
        for m in order:
            for f in range(2):
                at = (2 * pos[m] + f) * 128
                line = (1 - core if f else core) * nb + spot(m, "B")
                CL[0, pl.ds(line, 1), :] = ccol[:, at : at + 128]
        cc = [
            send(CL.at[0], CL.at[2 * m + f], cls.at[2 * m + f], clr.at[2 * m + f], peer(m, "B", f == 1))
            for m in reversed(order) for f in range(2) if m or f
        ]
        for c in cc:
            c.start()
        for m in order:
            at = slice(pos[m] * 128, (pos[m] + 1) * 128)
            tops = RM[at, :].T
            top = jnp.max(tops, axis=0, keepdims=True)
            part = jnp.sum(RS[at, :].T * jnp.exp2(tops - top), axis=0, keepdims=True)
            RL[0, pl.ds(spot(m, "A"), 1), :] = top + jnp.log2(part)
        rc = [send(RL.at[0], RL.at[m], rls.at[m], rlr.at[m], peer(m, "A")) for m in reversed(order[1:])]
        for c in rc:
            c.start()
    with jax.named_scope("turn"):
        def tilt(c, _):
            cols = pl.ds(pl.multiple_of(c * 256, 256), 256)
            cm = CM[:, cols]

            def strip(i, uc):
                at = pl.ds(pl.multiple_of(i * 256, 256), 256)
                v = L[at, cols]
                rm = RM[at, :]
                v0, v1 = v[:, :128], v[:, 128:]
                UR[at, :] = UR[at, :] + (jnp.exp2(v0 - rm) * v0 + jnp.exp2(v1 - rm) * v1)
                w = v.reshape(32, 8, 256)
                return uc + jnp.sum(jnp.exp2(w - cm) * w, axis=0)

            UC[:, cols] = lax.fori_loop(0, rows // 256, strip, jnp.zeros((8, 256), jnp.float32))
            return 0

        lax.fori_loop(0, nb, tilt, 0)
        XT[...] = X[...].T
        for c in started:
            c.wait_send()
    with jax.named_scope("lsewait"):
        for c in cc + rc:
            c.wait_recv()
        for c in cc + rc:
            c.wait_send()

    with jax.named_scope("join"):
        def joined(parts):
            top = functools.reduce(jnp.maximum, parts)
            return top + jnp.log2(functools.reduce(jnp.add, [jnp.exp2(p - top) for p in parts]))

        RL[0] = joined([RL[m] for m in range(nb)])
        CL[0] = joined([CL[m] for m in range(2 * nb)])
        for m in order:
            line = RL[0, pl.ds(spot(m, "A"), 1), :]
            RREP[pos[m] * 128 : (pos[m] + 1) * 128, :] = jnp.broadcast_to(line + 1.0, (128, 128)).T
            for f in range(2):
                at = (2 * pos[m] + f) * 128
                CROW[:, at : at + 128] = CL[0, pl.ds((1 - core if f else core) * nb + spot(m, "B"), 1), :] + 1.0
        eye = lax.broadcasted_iota(jnp.int32, (128, 128), 0) == lax.broadcasted_iota(jnp.int32, (128, 128), 1)
        paired = jnp.sum(jnp.where(eye, L[:128, :128], 0.0).reshape(16, 8, 128), axis=0)
        line = lax.broadcasted_iota(jnp.int32, (8, 128), 0)
        own = RL[0, pl.ds(spot(0, "A"), 1), :] + CL[0, pl.ds(core * nb + spot(0, "B"), 1), :]
        loss_part = jnp.where(line == 0, own, 0.0) - 2.0 * paired

    ip = cut(ROWS, nd, 8)
    tp = cut(XT.shape[0], nd, 8)

    def imsg(m, p):
        k = cube.hop(p, m)
        a, n = ip[p]
        at = pl.ds(pos[m] * ROWS + a, n)
        return send(PI.at[at], RI.at[at], pis.at[m, p], pir.at[m, p], peer(1 << k, "A"))

    def omsg(m, p):
        k = cube.hop(p, m)
        a, n = tp[p]
        at = pl.ds(a, n)
        return send(PT.at[0, pos[m], at], RT.at[pos[m], at], pts.at[m, p], ptr.at[m, p], peer(1 << k, "B"))

    def iadd(m, p):
        a, n = ip[p]
        v = PI[pos[m] * ROWS + a : pos[m] * ROWS + a + n, :]
        for c in cube.children(p, m):
            imsg(c, p).wait_recv()
            v = v + RI[pos[c] * ROWS + a : pos[c] * ROWS + a + n, :]
        PI[pos[m] * ROWS + a : pos[m] * ROWS + a + n, :] = v

    def oadd(m, p):
        a, n = tp[p]
        v = PT[0, pos[m], a : a + n, :]
        for c in cube.children(p, m):
            omsg(c, p).wait_recv()
            v = v + RT[pos[c], a : a + n, :]
        PT[0, pos[m], a : a + n, :] = v

    going = []

    def ready(m, msg):
        for p in cube.pieces:
            if m and not cube.children(p, m):
                c = msg(m, p)
                c.start()
                going.append(c)

    def follow(level, which):
        todo = [(m, p) for m in order if cube.level[m] == level for p in cube.pieces if cube.children(p, m)]
        for n in sorted({len(cube.children(p, m)) for m, p in todo}):
            for msg, add in [{"o": (omsg, oadd), "i": (imsg, iadd)}[w] for w in which]:
                for m, p in todo:
                    if len(cube.children(p, m)) == n:
                        add(m, p)
                        c = msg(m, p)
                        c.start()
                        going.append(c)

    pmsg = {
        m: send(PT.at[1, pos[m]], RTC.at[pos[m]], pcs.at[m], pcr.at[m], peer(0, "B", True)) for m in order
    }

    def pair(m):
        pmsg[m].wait_recv()
        PT[0, pos[m]] = PT[0, pos[m]] + RTC[pos[m]]
        ready(m, omsg)

    def weigh(r0, r1, c0, c1):
        for c in range(c0, c1):
            cols = slice(c * 256, (c + 1) * 256)
            cl = CROW[:, cols]
            for r in range(r0, r1, 64):
                at = slice(r, r + 64)
                v = L[at, cols]
                rl = RREP[at, :]
                w = jnp.exp2(v - jnp.concatenate([rl, rl], axis=1)) + jnp.exp2(v - cl)
                if c == 0 and r < 128:
                    across = lax.broadcasted_iota(jnp.int32, (64, 256), 1)
                    mark = lax.broadcasted_iota(jnp.int32, (64, 256), 0) + r == across
                    w = w - mark.astype(jnp.float32)
                W[at, cols] = w.astype(jnp.bfloat16)

    def text_grad(m):
        cols = slice(pos[m] * 256, (pos[m] + 1) * 256)
        v = jnp.dot(XT[...], W[:, cols], preferred_element_type=jnp.float32)
        PT[1, pos[m]] = v[:, 128:]
        PT[0, pos[m]] = v[:, :128]
        pmsg[m].start()

    def image_grad(first, last):
        at = slice(first * ROWS, last * ROWS)
        PI[at, :] = jnp.dot(W[at, :], T[...], preferred_element_type=jnp.float32)

    far = [(m, f) for m in range(nb) for f in (False, True) if m or f]
    stages = [
        [send(ST.at[0], ST.at[m], sts.at[m], str_.at[m], peer(m, "A")) for m in range(1, nb)],
        [send(ST.at[nb], ST.at[nb + 1 + i], sts.at[nb + i], str_.at[nb + i], peer(m, "B", f)) for i, (m, f) in enumerate(far)],
    ]

    def stat(at, copies):
        tile = ST[at]
        for j, c in enumerate(copies):
            c.wait_recv()
            tile = tile + ST[at + 1 + j]
        return tile

    def spread_scalars():
        part = -paired
        for r in range(0, rows, 128):
            at = slice(r, r + 128)
            part = part + jnp.sum((UR[at, :] * jnp.exp2(RM[at, :] - RREP[at, :])).reshape(16, 8, 128), axis=0)
        both = UC[...] * jnp.exp2(CM[...] - CROW[...])
        for c in range(0, 2 * rows, 128):
            part = part + both[:, c : c + 128]
        ST[0, :8] = loss_part
        ST[0, 8:] = part
        for c in stages[0]:
            c.start()

    spans = [(pos[ms[0]], pos[ms[-1]] + 1) for ms in levels]
    with jax.named_scope("farthest"):
        m = levels[nd][0]
        weigh(0, rows, pos[m], nb)
        text_grad(m)
        spread_scalars()
        weigh(pos[m] * ROWS, rows, 0, pos[m])
        image_grad(pos[m], nb)
        ready(m, imsg)
        waiting = [m]
    for lev in range(nd - 1, 1, -1):
        with jax.named_scope(f"middle{lev}"):
            first, last = spans[lev]
            weigh(0, last * ROWS, first, last)
            for m in levels[lev]:
                text_grad(m)
                if len(waiting) > 1 or waiting[0] == levels[nd][0]:
                    pair(waiting.pop(0))
                at = pos[m]
                weigh(at * ROWS, (at + 1) * ROWS, 0, first)
                image_grad(at, at + 1)
                ready(m, imsg)
                waiting.append(m)
            while waiting:
                pair(waiting.pop(0))
    with jax.named_scope("near"):
        first, last = spans[1] if nd > 1 else (1, 1)
        weigh(0, last * ROWS, 0, last)
        for m in levels[1] if nd > 1 else []:
            text_grad(m)
    with jax.named_scope("nearimages"):
        while waiting:
            pair(waiting.pop(0))
        if nd > 1:
            image_grad(first, last)
            follow(nd - 1, "i")
            for m in levels[1]:
                ready(m, imsg)
            follow(nd - 1, "o")
        for m in levels[1] if nd > 1 else []:
            pair(m)
    with jax.named_scope("stats"):
        ST[nb] = stat(0, stages[0])
        for c in stages[1]:
            c.start()
    with jax.named_scope("own"):
        text_grad(0)
        image_grad(0, 1)
    with jax.named_scope("follow"):
        for lev in range(nd - 2, 0, -1):
            follow(lev, "oi")
    with jax.named_scope("last"):
        for p in cube.pieces:
            iadd(0, p)
        gi_out[...] = (PI[:128, :] * scale[:, :1]).astype(jnp.bfloat16)
        tile = stat(nb, stages[1])
        loss = jnp.sum(tile[:8]) * (LN2 * 0.5 / total)
        grad_scale = jnp.sum(tile[8:]) * (LN2 / total)
        stats_out[...] = jnp.where(line == 0, loss, grad_scale)
    with jax.named_scope("lasttexts"):
        pair(0)
        for p in cube.pieces:
            oadd(0, p)
        gt_out[...] = (PT[0, 0] * scale).T.astype(jnp.bfloat16)
        for c in going + list(pmsg.values()) + stages[0] + stages[1]:
            c.wait_send()


def hand_over(gi, gt, stats, gi_out, gt_out, loss_out, scale_out):
    gi_out[...] = gi[...]
    gt_out[...] = gt[...]
    loss_out[...] = stats[0:1, 0:1]
    scale_out[...] = stats[1:2, 0:1]


def body(dims, total, images, texts, log_scale):
    nd = len(dims)
    nb = 2**nd
    f32, bf16 = jnp.float32, jnp.bfloat16
    vm, dma = pltpu.VMEM, pltpu.SemaphoreType.DMA
    width = images.shape[1]
    rows, cols = nb * ROWS, 2 * nb * ROWS
    gi, gt, stats = pl.pallas_call(
        functools.partial(kernel, dims, total),
        out_shape=(
            jax.ShapeDtypeStruct(images.shape, bf16),
            jax.ShapeDtypeStruct(texts.shape, bf16),
            jax.ShapeDtypeStruct((8, 128), f32),
        ),
        in_specs=[
            pl.BlockSpec(memory_space=pltpu.SMEM),
            pl.BlockSpec(memory_space=pl.ANY),
            pl.BlockSpec(memory_space=pl.ANY),
        ],
        out_specs=(pl.BlockSpec(memory_space=vm),) * 3,
        scratch_shapes=[
            vm((rows, width), bf16), vm((width, rows), bf16), vm((cols, width), bf16),
            vm((rows, cols), f32), vm((rows, cols), bf16),
            vm((rows, 128), f32), vm((rows, 128), f32), vm((rows, 128), f32), vm((rows, 128), f32),
            vm((8, cols), f32), vm((8, cols), f32), vm((8, cols), f32), vm((8, cols), f32),
            vm((nb, nb, 128), f32), vm((2 * nb, 2 * nb, 128), f32), vm((rows, 128), f32), vm((1, cols), f32),
            vm((rows, width), f32), vm((rows, width), f32),
            vm((2, nb, width, 128), f32), vm((nb, width, 128), f32), vm((nb, width, 128), f32),
            vm((3 * nb, 16, 128), f32),
            dma((2,)), dma((nb, nd)), dma((nb, nd)), dma((nb, nd)), dma((nb, nd)), dma((nb, nd)), dma((nb, nd)),
            dma((nb,)), dma((nb,)), dma((2 * nb,)), dma((2 * nb,)),
            dma((nb, nd)), dma((nb, nd)), dma((nb,)), dma((nb,)), dma((nb, nd)), dma((nb, nd)),
            dma((3 * nb,)), dma((3 * nb,)),
        ],
        compiler_params=pltpu.CompilerParams(
            collective_id=0, has_side_effects=True, vmem_limit_bytes=60 * 2**20
        ),
        name="contrastive",
    )(log_scale, images, texts)
    outs = pl.pallas_call(
        hand_over,
        out_shape=(
            jax.ShapeDtypeStruct(images.shape, bf16),
            jax.ShapeDtypeStruct(texts.shape, bf16),
            jax.ShapeDtypeStruct((1, 1), f32),
            jax.ShapeDtypeStruct((1, 1), f32),
        ),
        in_specs=[pl.BlockSpec(memory_space=vm)] * 3,
        out_specs=(pl.BlockSpec(memory_space=vm),) * 4,
        name="outputs",
    )(gi, gt, stats)
    return outs[0], outs[1], outs[2].reshape(()), outs[3].reshape(())


def solution(mesh):
    return build(Mesh(mesh.devices.reshape(4, 4, 2, 4), AXES))


def build(split):
    dims = tuple(a for a in CUBE if split.shape[a] == 4)
    placed = P(AXES, None)
    return jax.shard_map(
        functools.partial(body, dims, ROWS * split.size),
        mesh=split,
        in_specs=(placed, placed, P()),
        out_specs=(placed, placed, P(), P()),
        check_vma=False,
    )
```

```python
import functools
import math

import jax
import jax.numpy as jnp
from jax import lax
from jax.experimental import pallas as pl
from jax.experimental.pallas import tpu as pltpu
from jax.sharding import Mesh
from jax.sharding import PartitionSpec as P

AXES = ("x", "y", "core", "z")
CUBE = ("x", "y", "z")
MESH = pl.DeviceIdType.MESH
ROWS = 128
LOG2E = math.log2(math.e)
LN2 = math.log(2.0)
NT = (((1,), (1,)), ((), ()))


class Cube:
    def __init__(self, n):
        self.n = n
        self.order = sorted(range(2**n), key=lambda m: (bin(m).count("1"), m))
        self.pos = {m: i for i, m in enumerate(self.order)}
        self.level = {m: bin(m).count("1") for m in self.order}
        self.pieces = range(n)

    def hop(self, p, m):
        return next(k % self.n for k in range(p, p + self.n) if m >> (k % self.n) & 1)

    def children(self, p, m):
        more = [(k, m | 1 << k) for k in range(self.n) if not m >> k & 1]
        return [c for k, c in more if self.hop(p, c) == k]

    def turns(self):
        seen = []
        for q in (1, -1, 0):
            if q % self.n not in seen:
                seen.append(q % self.n)
        return seen


def cut(total, n, unit):
    units = total // unit
    ends = [-(-units * i // n) * unit for i in range(n + 1)]
    return [(a, b - a) for a, b in zip(ends, ends[1:])]


def kernel(
    dims, total,
    log_scale, images, texts,
    gi_out, gt_out, stats_out,
    X, XT, T, L, W, RM, RN, RS, UR, CM, CN, CS, UC, RL, CL, RREP, CROW,
    PI, RI, PT, RTC, RT, ST,
    local_sem, xs, xr, ts, tr, ds, dr, rls, rlr, cls, clr, pis, pir, pcs, pcr, pts, ptr, sts, str_,
):
    nd = len(dims)
    nb = 2**nd
    rows = nb * ROWS
    cube = Cube(nd)
    order, pos = cube.order, cube.pos
    me = {a: lax.axis_index(a) for a in AXES}
    core = me["core"]

    def peer(mask, kind, flip=False):
        ident = {}
        for d, a in enumerate(dims):
            if mask >> d & 1:
                c = me[a]
                ident[a] = 3 - c if kind == "A" else c + 1 - 2 * (c % 2)
        if flip:
            ident["core"] = 1 - core
        return ident

    def spot(mask, kind):
        at = 0
        for d, a in enumerate(dims):
            bit = me[a] // 2 if kind == "A" else me[a] % 2
            at = at + 2**d * (1 - bit if mask >> d & 1 else bit)
        return at

    def send(src, dst, s, r, where):
        return pltpu.make_async_remote_copy(
            src_ref=src, dst_ref=dst, send_sem=s, recv_sem=r, device_id=where, device_id_type=MESH
        )

    with jax.named_scope("enter"):
        ci = pltpu.make_async_copy(images, X.at[pl.ds(0, ROWS)], local_sem.at[0])
        ct = pltpu.make_async_copy(texts, T.at[pl.ds(0, ROWS)], local_sem.at[1])
        ci.start()
        ct.start()
        barrier = pltpu.get_barrier_semaphore()
        others = [(1 << k, kind, False) for k in range(nd) for kind in "AB"] + [(0, "B", True)]
        for o in others:
            pl.semaphore_signal(barrier, inc=1, device_id=peer(*o), device_id_type=MESH)
        RM[...] = jnp.full(RM.shape, -3e38, jnp.float32)
        RS[...] = jnp.zeros(RS.shape, jnp.float32)
        CM[...] = jnp.full(CM.shape, -3e38, jnp.float32)
        CS[...] = jnp.zeros(CS.shape, jnp.float32)
        UR[...] = jnp.zeros(UR.shape, jnp.float32)
        scale = jnp.exp(jnp.full((1, 128), log_scale[()], jnp.float32))
        scale_two = jnp.concatenate([scale * LOG2E] * 2, axis=1)
        ci.wait()
        ct.wait()
        pl.semaphore_wait(barrier, len(others))

    gp = cut(ROWS, nd, 16)
    started = []

    def go(c):
        c.start()
        started.append(c)

    def xmsg(m, p):
        k = cube.hop(p, m)
        a, n = gp[p]
        src = X.at[pl.ds(pos[m ^ 1 << k] * ROWS + a, n)]
        return send(src, X.at[pl.ds(pos[m] * ROWS + a, n)], xs.at[m, p], xr.at[m, p], peer(1 << k, "A"))

    def tmsg(m, p):
        k = cube.hop(p, m)
        a, n = gp[p]
        src = T.at[pl.ds(pos[m ^ 1 << k] * 2 * ROWS + a, n)]
        return send(src, T.at[pl.ds(pos[m] * 2 * ROWS + a, n)], ts.at[m, p], tr.at[m, p], peer(1 << k, "B"))

    def dmsg(m, p):
        a, n = gp[p]
        at = pos[m] * 2 * ROWS + a
        return send(T.at[pl.ds(at, n)], T.at[pl.ds(at + ROWS, n)], ds.at[m, p], dr.at[m, p], peer(0, "B", True))

    def pass_on(events):
        nxt = [(c, p) for m, p in events for c in cube.children(p, m)]
        nxt.sort(key=lambda e: not cube.children(e[1], e[0]))
        for m, p in events:
            tmsg(m, p).wait_recv()
        for e in nxt:
            go(tmsg(*e))
        for e in events:
            go(dmsg(*e))
        for m, p in events:
            xmsg(m, p).wait_recv()
        for e in nxt:
            go(xmsg(*e))

    def logits(r0, r1, c0, c1):
        for i in range(c0, c1):
            cols = slice(i * 256, (i + 1) * 256)
            v = lax.dot_general(X[r0:r1, :], T[cols, :], NT, preferred_element_type=jnp.float32) * scale_two
            L[r0:r1, cols] = v
            RN[r0:r1, :] = jnp.maximum(RN[r0:r1, :], jnp.maximum(v[:, :128], v[:, 128:]))
            CN[:, cols] = jnp.maximum(CN[:, cols], jnp.max(v.reshape(-1, 8, 256), axis=0))

    def new_tops(r0, r1, c0, c1):
        at = slice(r0, r1)
        RS[at, :] = RS[at, :] * jnp.exp2(RM[at, :] - RN[at, :])
        RM[at, :] = RN[at, :]
        cols = slice(c0 * 256, c1 * 256)
        CS[:, cols] = CS[:, cols] * jnp.exp2(CM[:, cols] - CN[:, cols])
        CM[:, cols] = CN[:, cols]

    def sums(r0, r1, c0, c1):
        def step(i, _):
            cols = pl.ds(pl.multiple_of(i * 256, 256), 256)
            cm = CM[:, cols]
            cs = CS[:, cols]
            for r in range(r0, r1, 64):
                at = slice(r, r + 64)
                v = L[at, cols]
                rm = RM[at, :]
                er0 = jnp.exp2(v[:, :128] - rm)
                er1 = jnp.exp2(v[:, 128:] - rm)
                RS[at, :] = RS[at, :] + (er0 + er1)
                ec = jnp.exp2(v.reshape(8, 8, 256) - cm)
                cs = cs + jnp.sum(ec, axis=0)
            CS[:, cols] = cs
            return 0

        lax.fori_loop(c0, c1, step, 0)

    def partner_texts(masks):
        for m in masks:
            for p in cube.pieces:
                dmsg(m, p).wait_recv()

    with jax.named_scope("gather"):
        for p in cube.pieces:
            go(dmsg(0, p))
        for q in cube.turns():
            for k in range(nd):
                go(xmsg(1 << k, (k + q) % nd))
                go(tmsg(1 << k, (k + q) % nd))
        levels = [[m for m in order if cube.level[m] == i] for i in range(nd + 1)]
        RN[...] = RM[...]
        CN[...] = CM[...]
        partner_texts(levels[0])
        logits(0, ROWS, 0, 1)
        new_tops(0, ROWS, 0, 1)
        sums(0, ROWS, 0, 1)
        groups = [[(1 << k, (k + q) % nd) for k in range(nd)] for q in cube.turns()]
        for g in groups:
            pass_on(g)
    for lev in range(1, nd + 1):
        before = sum(len(levels[i]) for i in range(lev))
        done = before + len(levels[lev])
        old, new = before * ROWS, done * ROWS
        with jax.named_scope(f"gather{lev}"):
            if 1 < lev < nd:
                events = [(m, p) for m in levels[lev] for p in cube.pieces]
                deep = [e for e in events if cube.children(e[1], e[0])]
                if deep:
                    pass_on(deep)
                pass_on([e for e in events if e not in deep])
            elif lev > 1:
                pass_on([(m, p) for m in levels[lev] for p in cube.pieces])
        with jax.named_scope(f"rows{lev}"):
            logits(old, new, 0, before)
            new_tops(old, new, 0, before)
            sums(old, new, 0, before)
        with jax.named_scope(f"partner{lev}"):
            partner_texts(levels[lev])
        with jax.named_scope(f"columns{lev}"):
            logits(0, new, before, done)
            new_tops(0, new, before, done)
            sums(0, new, before, done)

    with jax.named_scope("lse"):
        for m in order:
            at = slice(pos[m] * 128, (pos[m] + 1) * 128)
            tops = RM[at, :].T
            top = jnp.max(tops, axis=0, keepdims=True)
            part = jnp.sum(RS[at, :].T * jnp.exp2(tops - top), axis=0, keepdims=True)
            RL[0, pl.ds(spot(m, "A"), 1), :] = top + jnp.log2(part)
        rc = [send(RL.at[0], RL.at[m], rls.at[m], rlr.at[m], peer(m, "A")) for m in reversed(order[1:])]
        for c in rc:
            c.start()
        ctop = jnp.max(CM[...], axis=0, keepdims=True)
        ccol = ctop + jnp.log2(jnp.sum(CS[...] * jnp.exp2(CM[...] - ctop), axis=0, keepdims=True))
        for m in order:
            for f in range(2):
                at = (2 * pos[m] + f) * 128
                line = (1 - core if f else core) * nb + spot(m, "B")
                CL[0, pl.ds(line, 1), :] = ccol[:, at : at + 128]
        cc = [
            send(CL.at[0], CL.at[2 * m + f], cls.at[2 * m + f], clr.at[2 * m + f], peer(m, "B", f == 1))
            for m in reversed(order) for f in range(2) if m or f
        ]
        for c in cc:
            c.start()
    with jax.named_scope("turn"):
        def tilt(c, _):
            cols = pl.ds(pl.multiple_of(c * 256, 256), 256)
            cm = CM[:, cols]

            def strip(i, uc):
                at = pl.ds(pl.multiple_of(i * 256, 256), 256)
                v = L[at, cols]
                rm = RM[at, :]
                v0, v1 = v[:, :128], v[:, 128:]
                UR[at, :] = UR[at, :] + (jnp.exp2(v0 - rm) * v0 + jnp.exp2(v1 - rm) * v1)
                w = v.reshape(32, 8, 256)
                return uc + jnp.sum(jnp.exp2(w - cm) * w, axis=0)

            UC[:, cols] = lax.fori_loop(0, rows // 256, strip, jnp.zeros((8, 256), jnp.float32))
            return 0

        lax.fori_loop(0, nb, tilt, 0)
        XT[...] = X[...].T
        for c in started:
            c.wait_send()
    with jax.named_scope("lsewait"):
        for c in cc + rc:
            c.wait_recv()
        for c in cc + rc:
            c.wait_send()

    with jax.named_scope("join"):
        def joined(parts):
            top = functools.reduce(jnp.maximum, parts)
            return top + jnp.log2(functools.reduce(jnp.add, [jnp.exp2(p - top) for p in parts]))

        RL[0] = joined([RL[m] for m in range(nb)])
        CL[0] = joined([CL[m] for m in range(2 * nb)])
        for m in order:
            line = RL[0, pl.ds(spot(m, "A"), 1), :]
            RREP[pos[m] * 128 : (pos[m] + 1) * 128, :] = jnp.broadcast_to(line + 1.0, (128, 128)).T
            for f in range(2):
                at = (2 * pos[m] + f) * 128
                CROW[:, at : at + 128] = CL[0, pl.ds((1 - core if f else core) * nb + spot(m, "B"), 1), :] + 1.0
        eye = lax.broadcasted_iota(jnp.int32, (128, 128), 0) == lax.broadcasted_iota(jnp.int32, (128, 128), 1)
        paired = jnp.sum(jnp.where(eye, L[:128, :128], 0.0).reshape(16, 8, 128), axis=0)
        line = lax.broadcasted_iota(jnp.int32, (8, 128), 0)
        own = RL[0, pl.ds(spot(0, "A"), 1), :] + CL[0, pl.ds(core * nb + spot(0, "B"), 1), :]
        loss_part = jnp.where(line == 0, own, 0.0) - 2.0 * paired

    ip = cut(ROWS, nd, 8)
    tp = cut(XT.shape[0], nd, 8)

    def imsg(m, p):
        k = cube.hop(p, m)
        a, n = ip[p]
        at = pl.ds(pos[m] * ROWS + a, n)
        return send(PI.at[at], RI.at[at], pis.at[m, p], pir.at[m, p], peer(1 << k, "A"))

    def omsg(m, p):
        k = cube.hop(p, m)
        a, n = tp[p]
        at = pl.ds(a, n)
        return send(PT.at[0, pos[m], at], RT.at[pos[m], at], pts.at[m, p], ptr.at[m, p], peer(1 << k, "B"))

    def iadd(m, p):
        a, n = ip[p]
        v = PI[pos[m] * ROWS + a : pos[m] * ROWS + a + n, :]
        for c in cube.children(p, m):
            imsg(c, p).wait_recv()
            v = v + RI[pos[c] * ROWS + a : pos[c] * ROWS + a + n, :]
        PI[pos[m] * ROWS + a : pos[m] * ROWS + a + n, :] = v

    def oadd(m, p):
        a, n = tp[p]
        v = PT[0, pos[m], a : a + n, :]
        for c in cube.children(p, m):
            omsg(c, p).wait_recv()
            v = v + RT[pos[c], a : a + n, :]
        PT[0, pos[m], a : a + n, :] = v

    going = []

    def ready(m, msg):
        for p in cube.pieces:
            if m and not cube.children(p, m):
                c = msg(m, p)
                c.start()
                going.append(c)

    def follow(level, which):
        todo = [(m, p) for m in order if cube.level[m] == level for p in cube.pieces if cube.children(p, m)]
        for n in sorted({len(cube.children(p, m)) for m, p in todo}):
            for msg, add in [{"o": (omsg, oadd), "i": (imsg, iadd)}[w] for w in which]:
                for m, p in todo:
                    if len(cube.children(p, m)) == n:
                        add(m, p)
                        c = msg(m, p)
                        c.start()
                        going.append(c)

    pmsg = {
        m: send(PT.at[1, pos[m]], RTC.at[pos[m]], pcs.at[m], pcr.at[m], peer(0, "B", True)) for m in order
    }

    def pair(m):
        pmsg[m].wait_recv()
        PT[0, pos[m]] = PT[0, pos[m]] + RTC[pos[m]]
        ready(m, omsg)

    def weigh(r0, r1, c0, c1):
        for c in range(c0, c1):
            cols = slice(c * 256, (c + 1) * 256)
            cl = CROW[:, cols]
            for r in range(r0, r1, 64):
                at = slice(r, r + 64)
                v = L[at, cols]
                rl = RREP[at, :]
                w = jnp.exp2(v - jnp.concatenate([rl, rl], axis=1)) + jnp.exp2(v - cl)
                if c == 0 and r < 128:
                    across = lax.broadcasted_iota(jnp.int32, (64, 256), 1)
                    mark = lax.broadcasted_iota(jnp.int32, (64, 256), 0) + r == across
                    w = w - mark.astype(jnp.float32)
                W[at, cols] = w.astype(jnp.bfloat16)

    def text_grad(m):
        cols = slice(pos[m] * 256, (pos[m] + 1) * 256)
        v = jnp.dot(XT[...], W[:, cols], preferred_element_type=jnp.float32)
        PT[1, pos[m]] = v[:, 128:]
        PT[0, pos[m]] = v[:, :128]
        pmsg[m].start()

    def image_grad(first, last):
        at = slice(first * ROWS, last * ROWS)
        PI[at, :] = jnp.dot(W[at, :], T[...], preferred_element_type=jnp.float32)

    far = [(m, f) for m in range(nb) for f in (False, True) if m or f]
    stages = [
        [send(ST.at[0], ST.at[m], sts.at[m], str_.at[m], peer(m, "A")) for m in range(1, nb)],
        [send(ST.at[nb], ST.at[nb + 1 + i], sts.at[nb + i], str_.at[nb + i], peer(m, "B", f)) for i, (m, f) in enumerate(far)],
    ]

    def stat(at, copies):
        tile = ST[at]
        for j, c in enumerate(copies):
            c.wait_recv()
            tile = tile + ST[at + 1 + j]
        return tile

    def spread_scalars():
        part = -paired
        for r in range(0, rows, 128):
            at = slice(r, r + 128)
            part = part + jnp.sum((UR[at, :] * jnp.exp2(RM[at, :] - RREP[at, :])).reshape(16, 8, 128), axis=0)
        both = UC[...] * jnp.exp2(CM[...] - CROW[...])
        for c in range(0, 2 * rows, 128):
            part = part + both[:, c : c + 128]
        ST[0, :8] = loss_part
        ST[0, 8:] = part
        for c in stages[0]:
            c.start()

    spans = [(pos[ms[0]], pos[ms[-1]] + 1) for ms in levels]
    with jax.named_scope("farthest"):
        m = levels[nd][0]
        weigh(0, rows, pos[m], nb)
        text_grad(m)
        spread_scalars()
        weigh(pos[m] * ROWS, rows, 0, pos[m])
        image_grad(pos[m], nb)
        ready(m, imsg)
        waiting = [m]
    for lev in range(nd - 1, 1, -1):
        with jax.named_scope(f"middle{lev}"):
            first, last = spans[lev]
            weigh(0, last * ROWS, first, last)
            for m in levels[lev]:
                text_grad(m)
                if len(waiting) > 1 or waiting[0] == levels[nd][0]:
                    pair(waiting.pop(0))
                at = pos[m]
                weigh(at * ROWS, (at + 1) * ROWS, 0, first)
                image_grad(at, at + 1)
                ready(m, imsg)
                waiting.append(m)
            while waiting:
                pair(waiting.pop(0))
    with jax.named_scope("near"):
        first, last = spans[1] if nd > 1 else (1, 1)
        weigh(0, last * ROWS, 0, last)
        for m in levels[1] if nd > 1 else []:
            text_grad(m)
    with jax.named_scope("nearimages"):
        while waiting:
            pair(waiting.pop(0))
        if nd > 1:
            image_grad(first, last)
            follow(nd - 1, "i")
            for m in levels[1]:
                ready(m, imsg)
            follow(nd - 1, "o")
        for m in levels[1] if nd > 1 else []:
            pair(m)
    with jax.named_scope("stats"):
        ST[nb] = stat(0, stages[0])
        for c in stages[1]:
            c.start()
    with jax.named_scope("own"):
        text_grad(0)
        image_grad(0, 1)
    with jax.named_scope("follow"):
        for lev in range(nd - 2, 0, -1):
            follow(lev, "oi")
    with jax.named_scope("last"):
        for p in cube.pieces:
            iadd(0, p)
        gi_out[...] = (PI[:128, :] * scale[:, :1]).astype(jnp.bfloat16)
        tile = stat(nb, stages[1])
        loss = jnp.sum(tile[:8]) * (LN2 * 0.5 / total)
        grad_scale = jnp.sum(tile[8:]) * (LN2 / total)
        stats_out[...] = jnp.where(line == 0, loss, grad_scale)
    with jax.named_scope("lasttexts"):
        pair(0)
        for p in cube.pieces:
            oadd(0, p)
        gt_out[...] = (PT[0, 0] * scale).T.astype(jnp.bfloat16)
        for c in going + list(pmsg.values()) + stages[0] + stages[1]:
            c.wait_send()


def hand_over(gi, gt, stats, gi_out, gt_out, loss_out, scale_out):
    gi_out[...] = gi[...]
    gt_out[...] = gt[...]
    loss_out[...] = stats[0:1, 0:1]
    scale_out[...] = stats[1:2, 0:1]


def body(dims, total, images, texts, log_scale):
    nd = len(dims)
    nb = 2**nd
    f32, bf16 = jnp.float32, jnp.bfloat16
    vm, dma = pltpu.VMEM, pltpu.SemaphoreType.DMA
    width = images.shape[1]
    rows, cols = nb * ROWS, 2 * nb * ROWS
    gi, gt, stats = pl.pallas_call(
        functools.partial(kernel, dims, total),
        out_shape=(
            jax.ShapeDtypeStruct(images.shape, bf16),
            jax.ShapeDtypeStruct(texts.shape, bf16),
            jax.ShapeDtypeStruct((8, 128), f32),
        ),
        in_specs=[
            pl.BlockSpec(memory_space=pltpu.SMEM),
            pl.BlockSpec(memory_space=pl.ANY),
            pl.BlockSpec(memory_space=pl.ANY),
        ],
        out_specs=(pl.BlockSpec(memory_space=vm),) * 3,
        scratch_shapes=[
            vm((rows, width), bf16), vm((width, rows), bf16), vm((cols, width), bf16),
            vm((rows, cols), f32), vm((rows, cols), bf16),
            vm((rows, 128), f32), vm((rows, 128), f32), vm((rows, 128), f32), vm((rows, 128), f32),
            vm((8, cols), f32), vm((8, cols), f32), vm((8, cols), f32), vm((8, cols), f32),
            vm((nb, nb, 128), f32), vm((2 * nb, 2 * nb, 128), f32), vm((rows, 128), f32), vm((1, cols), f32),
            vm((rows, width), f32), vm((rows, width), f32),
            vm((2, nb, width, 128), f32), vm((nb, width, 128), f32), vm((nb, width, 128), f32),
            vm((3 * nb, 16, 128), f32),
            dma((2,)), dma((nb, nd)), dma((nb, nd)), dma((nb, nd)), dma((nb, nd)), dma((nb, nd)), dma((nb, nd)),
            dma((nb,)), dma((nb,)), dma((2 * nb,)), dma((2 * nb,)),
            dma((nb, nd)), dma((nb, nd)), dma((nb,)), dma((nb,)), dma((nb, nd)), dma((nb, nd)),
            dma((3 * nb,)), dma((3 * nb,)),
        ],
        compiler_params=pltpu.CompilerParams(
            collective_id=0, has_side_effects=True, vmem_limit_bytes=60 * 2**20
        ),
        name="contrastive",
    )(log_scale, images, texts)
    outs = pl.pallas_call(
        hand_over,
        out_shape=(
            jax.ShapeDtypeStruct(images.shape, bf16),
            jax.ShapeDtypeStruct(texts.shape, bf16),
            jax.ShapeDtypeStruct((1, 1), f32),
            jax.ShapeDtypeStruct((1, 1), f32),
        ),
        in_specs=[pl.BlockSpec(memory_space=vm)] * 3,
        out_specs=(pl.BlockSpec(memory_space=vm),) * 4,
        name="outputs",
    )(gi, gt, stats)
    return outs[0], outs[1], outs[2].reshape(()), outs[3].reshape(())


def solution(mesh):
    return build(Mesh(mesh.devices.reshape(4, 4, 2, 4), AXES))


def build(split):
    dims = tuple(a for a in CUBE if split.shape[a] == 4)
    placed = P(AXES, None)
    return jax.shard_map(
        functools.partial(body, dims, ROWS * split.size),
        mesh=split,
        in_specs=(placed, placed, P()),
        out_specs=(placed, placed, P(), P()),
        check_vma=False,
    )
```
